32 devices in a mesh: data: 1 (over z), cp: 4 (over y), tp: 8 (over x, core).
Axes of the slice: x: 4, y: 4, z: 1, core: 2. Of those that a mesh axis runs over, the one named last changes fastest.
The devices are a block of a 4x4x8 slice.
Arguments:
- act_in: bfloat16 [2, 4096, 2048], P(None, ('data', 'cp', 'tp'))
- route_ids: int32 [2, 4096, 2], P(None, ('data', 'cp', 'tp'))
- route_gates: float32 [2, 4096, 2], P(None, ('data', 'cp', 'tp'))
- w_query: bfloat16 [2048, 16, 128], P(None, 'tp')
- w_key: bfloat16 [2048, 16, 128], P(None, 'tp')
- w_value: bfloat16 [2048, 16, 128], P(None, 'tp')
- w_out: bfloat16 [16, 128, 2048], P('tp')
- w_gate: bfloat16 [32, 2048, 1408], P(('cp', 'tp'))
- w_up: bfloat16 [32, 2048, 1408], P(('cp', 'tp'))
- w_down: bfloat16 [32, 1408, 2048], P(('cp', 'tp'))
Outputs:
- output: bfloat16 [2, 4096, 2048], P(None, ('data', 'cp', 'tp'))
All inputs are finite; a program needn't handle non-finite values.
Results may differ from the reference program's by a relative error of at most 0.00522276.
Values are sent between devices in bfloat16 or wider.
A program may use at most 768 MiB of HBM per device.

```python
import math
import jax
import jax.numpy as jnp
from jax import lax

HIDDEN = 2048
EXPERT_FF = 1408
Q_HEADS = 16
KV_HEADS = 16
HEAD_DIM = 128
CP_SIZE = 4
TP_SIZE = 8
TOKENS_DEV = 128
MICRO_BATCHES = 2

EXPERTS = CP_SIZE * TP_SIZE
SEQ_LEN = TOKENS_DEV * EXPERTS
PIECE_LEN = SEQ_LEN // (2 * CP_SIZE)
CAPACITY = (4 * TOKENS_DEV) // EXPERTS
EXPERT_ROWS = CAPACITY * EXPERTS
GROUP_SIZE = Q_HEADS // KV_HEADS
SCORE_SHARP = math.sqrt(0.75 * math.log(SEQ_LEN))


def draw_routing(base_key):
    half_cap = CAPACITY // 2

    def one_source(src_key):
        k_perm, k_delta, k_tok, k_swap = jax.random.split(src_key, 4)
        expert_perm = jax.random.permutation(k_perm, EXPERTS)
        deltas = jax.random.randint(k_delta, (EXPERTS // 2,), 0, half_cap + 1).at[0].set(half_cap)
        pair_counts = jnp.stack([half_cap + deltas, half_cap - deltas], axis=1).reshape(EXPERTS)
        counts = jnp.zeros((EXPERTS,), jnp.int32).at[expert_perm].set(pair_counts)
        count_ends = jnp.cumsum(counts)
        labels = jnp.sum((jnp.arange(2 * TOKENS_DEV)[:, None] >= count_ends[None, :]).astype(jnp.int32), axis=1)
        id_pairs = jnp.stack([labels[:TOKENS_DEV], labels[TOKENS_DEV:]], axis=1)
        id_pairs = id_pairs[jax.random.permutation(k_tok, TOKENS_DEV)]
        swap_flag = jax.random.randint(k_swap, (TOKENS_DEV, 1), 0, 2)
        return jnp.where(swap_flag == 1, id_pairs[:, ::-1], id_pairs).astype(jnp.int32)

    return jax.vmap(one_source)(jax.random.split(base_key, EXPERTS)).reshape(SEQ_LEN, 2)


def normal_weight(weight_key, arr_shape, w_scale):
    return (jax.random.normal(weight_key, arr_shape, jnp.float32) * w_scale).astype(jnp.bfloat16)


def expert_stack(weight_key, arr_shape, w_scale):
    return lax.map(lambda one_key: normal_weight(one_key, arr_shape, w_scale), jax.random.split(weight_key, EXPERTS))


def setup_inputs(seed: int = 0, part: int = 0) -> dict:
    part_key = jax.random.fold_in(jax.random.key(seed), part)
    k_act, k_route, k_gate = jax.random.split(part_key, 3)
    shared = jax.random.split(jax.random.key(seed + 1), 7)
    act_in = jax.random.normal(k_act, (MICRO_BATCHES, SEQ_LEN, HIDDEN), jnp.float32).astype(jnp.bfloat16)
    route_ids = jax.vmap(draw_routing)(jax.random.split(k_route, MICRO_BATCHES))
    route_gates = jax.random.uniform(k_gate, (MICRO_BATCHES, SEQ_LEN, 2), jnp.float32, 0.3, 0.7)
    return {
        'act_in': act_in,
        'route_ids': route_ids,
        'route_gates': route_gates,
        'w_query': normal_weight(shared[0], (HIDDEN, Q_HEADS, HEAD_DIM), SCORE_SHARP / math.sqrt(HIDDEN)),
        'w_key': normal_weight(shared[1], (HIDDEN, KV_HEADS, HEAD_DIM), 1.0 / math.sqrt(HIDDEN)),
        'w_value': normal_weight(shared[2], (HIDDEN, KV_HEADS, HEAD_DIM), 1.0 / math.sqrt(HIDDEN)),
        'w_out': normal_weight(shared[3], (Q_HEADS, HEAD_DIM, HIDDEN), 1.0 / math.sqrt(Q_HEADS * HEAD_DIM)),
        'w_gate': expert_stack(shared[4], (HIDDEN, EXPERT_FF), 1.0 / math.sqrt(HIDDEN)),
        'w_up': expert_stack(shared[5], (HIDDEN, EXPERT_FF), 1.0 / math.sqrt(HIDDEN)),
        'w_down': expert_stack(shared[6], (EXPERT_FF, HIDDEN), 1.0 / math.sqrt(EXPERT_FF)),
    }


def token_positions():
    row_ix = jnp.arange(SEQ_LEN)
    owner_ix = row_ix // (2 * PIECE_LEN)
    inner_ix = row_ix % (2 * PIECE_LEN)
    return jnp.where(inner_ix < PIECE_LEN, owner_ix * PIECE_LEN + inner_ix, (2 * CP_SIZE - 1 - owner_ix) * PIECE_LEN + inner_ix - PIECE_LEN)


def attention_block(seq_in, w_query, w_key, w_value, w_out):
    query_rows = jnp.dot(seq_in, w_query.reshape(HIDDEN, Q_HEADS * HEAD_DIM), preferred_element_type=jnp.float32).astype(jnp.bfloat16)
    key_rows = jnp.dot(seq_in, w_key.reshape(HIDDEN, KV_HEADS * HEAD_DIM), preferred_element_type=jnp.float32).astype(jnp.bfloat16)
    value_rows = jnp.dot(seq_in, w_value.reshape(HIDDEN, KV_HEADS * HEAD_DIM), preferred_element_type=jnp.float32).astype(jnp.bfloat16)
    key_rows = key_rows.astype(jnp.float32).reshape(SEQ_LEN, KV_HEADS, HEAD_DIM)
    value_rows = value_rows.astype(jnp.float32).reshape(SEQ_LEN, KV_HEADS, HEAD_DIM)
    positions = token_positions()
    query_blocks = query_rows.reshape(EXPERTS, TOKENS_DEV, KV_HEADS, GROUP_SIZE, HEAD_DIM)
    pos_blocks = positions.reshape(EXPERTS, TOKENS_DEV)

    def one_block(block_args):
        q_block, q_pos = block_args
        scores = jnp.einsum('qhgd,khd->hgqk', q_block.astype(jnp.float32), key_rows) * HEAD_DIM ** -0.5
        scores = jnp.where(positions[None, :] <= q_pos[:, None], scores, -jnp.inf)
        row_peak = jnp.max(scores, axis=-1, keepdims=True)
        exp_scores = jnp.exp(scores - row_peak)
        row_sum = jnp.sum(exp_scores, axis=-1)
        weighted = jnp.einsum('hgqk,khd->qhgd', exp_scores.astype(jnp.bfloat16).astype(jnp.float32), value_rows)
        weighted = weighted / jnp.transpose(row_sum, (2, 0, 1))[..., None]
        return weighted.astype(jnp.bfloat16).reshape(TOKENS_DEV, Q_HEADS * HEAD_DIM)

    attn_rows = lax.map(one_block, (query_blocks, pos_blocks)).reshape(SEQ_LEN, Q_HEADS * HEAD_DIM)
    attn_sum = jnp.dot(attn_rows, w_out.reshape(Q_HEADS * HEAD_DIM, HIDDEN), preferred_element_type=jnp.float32)
    return (seq_in.astype(jnp.float32) + attn_sum).astype(jnp.bfloat16)


def expert_block(mid_rows, seq_ids, seq_gates, w_gate, w_up, w_down):
    choice_expert = seq_ids.reshape(2 * SEQ_LEN)
    choice_token = jnp.arange(2 * SEQ_LEN) // 2
    sort_ix = jnp.argsort(choice_expert, stable=True)
    counts = jnp.sum((choice_expert[None, :] == jnp.arange(EXPERTS)[:, None]).astype(jnp.int32), axis=1)
    starts = jnp.cumsum(counts) - counts
    sorted_token = jnp.concatenate([choice_token[sort_ix], jnp.zeros((EXPERT_ROWS,), choice_token.dtype)])

    def one_expert(expert_id):
        token_ids = lax.dynamic_slice(sorted_token, (starts[expert_id],), (EXPERT_ROWS,))
        expert_in = mid_rows[token_ids]
        gate_act = jnp.dot(expert_in, w_gate[expert_id], preferred_element_type=jnp.float32)
        up_act = jnp.dot(expert_in, w_up[expert_id], preferred_element_type=jnp.float32)
        mixed_act = (jax.nn.silu(gate_act) * up_act).astype(jnp.bfloat16)
        return jnp.dot(mixed_act, w_down[expert_id], preferred_element_type=jnp.float32).astype(jnp.bfloat16)

    expert_out = lax.map(one_expert, jnp.arange(EXPERTS)).reshape(EXPERTS * EXPERT_ROWS, HIDDEN)
    sorted_expert = choice_expert[sort_ix]
    slot_rank = jnp.arange(2 * SEQ_LEN) - starts[sorted_expert]
    z_sorted = expert_out[sorted_expert * EXPERT_ROWS + slot_rank]
    z_choice = z_sorted[jnp.argsort(sort_ix)].reshape(SEQ_LEN, 2, HIDDEN)
    mixed_sum = jnp.sum(seq_gates[:, :, None] * z_choice.astype(jnp.float32), axis=1)
    return (mid_rows.astype(jnp.float32) + mixed_sum).astype(jnp.bfloat16)


def reference(act_in, route_ids, route_gates, w_query, w_key, w_value, w_out, w_gate, w_up, w_down):
    def one_sequence(seq_args):
        seq_in, seq_ids, seq_gates = seq_args
        mid_rows = attention_block(seq_in, w_query, w_key, w_value, w_out)
        return expert_block(mid_rows, seq_ids, seq_gates, w_gate, w_up, w_down)

    return lax.map(one_sequence, (act_in, route_ids, route_gates))
```

```python
import functools

import jax
import jax.numpy as jnp
from jax import lax
from jax.experimental import pallas as pl
from jax.experimental.pallas import tpu as pltpu
from jax.sharding import PartitionSpec as P

LOG2E = 1.4426950408889634


def attention_body(pieces, piece_len, head_dim, qkv_ref, o_ref, s_ref):
    p = pl.program_id(0)
    half = pieces // 2
    factor = head_dim ** -0.5 * LOG2E

    def offset(n):
        return pl.multiple_of(jnp.where(n < half, 2 * piece_len * n, 2 * piece_len * (pieces - 1 - n) + piece_len), piece_len)

    q_rows = qkv_ref[pl.ds(offset(p), piece_len), 0:head_dim]

    def scores(n):
        k_rows = qkv_ref[pl.ds(offset(n), piece_len), head_dim:2 * head_dim]
        return lax.dot_general(q_rows, k_rows, (((1,), (1,)), ((), ())), preferred_element_type=jnp.float32)

    def fold(op, wide):
        parts = [wide[:, i * 128:(i + 1) * 128] for i in range(piece_len // 128)]
        while len(parts) > 1:
            parts = [op(a, b) for a, b in zip(parts[::2], parts[1::2])]
        return parts[0]

    def first(n, peak):
        s = scores(n)
        s_ref[n] = s
        return jnp.maximum(peak, fold(jnp.maximum, s))

    row = lax.broadcasted_iota(jnp.int32, (piece_len, piece_len), 0)
    col = lax.broadcasted_iota(jnp.int32, (piece_len, piece_len), 1)
    s_diag = jnp.where(col <= row, scores(p), -jnp.inf)
    s_ref[p] = s_diag
    peak = lax.fori_loop(0, p, first, fold(jnp.maximum, s_diag))
    peak = jnp.max(peak, axis=1, keepdims=True) * factor

    def second(n, carry):
        total, acc = carry
        e = jnp.exp2(s_ref[n] * factor - peak)
        v_rows = qkv_ref[pl.ds(offset(n), piece_len), 2 * head_dim:3 * head_dim]
        acc = acc + jnp.dot(e.astype(jnp.bfloat16), v_rows, preferred_element_type=jnp.float32)
        return total + fold(jnp.add, e), acc

    zero = jnp.zeros((piece_len, 128), jnp.float32)
    total, acc = lax.fori_loop(0, p + 1, second, (zero, jnp.zeros((piece_len, head_dim), jnp.float32)))
    total = jnp.sum(total, axis=1, keepdims=True)
    o_ref[pl.ds(offset(p), piece_len), :] = (acc / total).astype(jnp.bfloat16)


def attend_unit(qkv, pieces):
    rows, width = qkv.shape
    head_dim = width // 3
    piece_len = rows // pieces
    return pl.pallas_call(
        functools.partial(attention_body, pieces, piece_len, head_dim),
        grid=(pieces,),
        out_shape=jax.ShapeDtypeStruct((rows, head_dim), jnp.bfloat16),
        in_specs=[pl.BlockSpec((rows, width), lambda p: (0, 0))],
        out_specs=pl.BlockSpec((rows, head_dim), lambda p: (0, 0)),
        scratch_shapes=[pltpu.VMEM((pieces, piece_len, piece_len), jnp.float32)],
        compiler_params=pltpu.CompilerParams(vmem_limit_bytes=40 << 20),
        cost_estimate=pl.CostEstimate(flops=9 * 4 * rows * rows * head_dim // 16, bytes_accessed=4 * rows * head_dim * 2, transcendentals=0),
    )(qkv)


def solution(mesh):
    cp_size = mesh.shape['cp']
    tp_size = mesh.shape['tp']
    experts = cp_size * tp_size
    row_spec = P(None, ('data', 'cp', 'tp'), None)
    head_spec = P(None, 'tp', None)
    out_spec = P('tp', None, None)
    expert_spec = P(('cp', 'tp'), None, None)

    def device_step(act_in, route_ids, route_gates, w_query, w_key, w_value, w_out, w_gate, w_up, w_down):
        n_micro, tokens, hidden = act_in.shape
        heads, head_dim = w_query.shape[1], w_query.shape[2]
        half_rows = tokens * tp_size
        w_qkv = jnp.concatenate([w_query, w_key, w_value], axis=2)
        x_half = lax.all_gather(act_in, 'tp', axis=1, tiled=True)
        w_full = lax.all_gather(w_out, 'tp', axis=0, tiled=True)
        qkv = jnp.einsum('bsh,hnd->bnsd', x_half, w_qkv, preferred_element_type=jnp.float32).astype(jnp.bfloat16)
        unit = lax.all_to_all(qkv.reshape(n_micro * heads, half_rows, 3 * head_dim), 'cp', 0, 0, tiled=True)
        o_unit = attend_unit(unit.reshape(cp_size * half_rows, 3 * head_dim), 2 * cp_size)
        o_recv = lax.all_to_all(o_unit.reshape(experts, tokens, head_dim), ('cp', 'tp'), 0, 0, tiled=True)
        o_rows = o_recv.reshape(n_micro, heads, tp_size, tokens, head_dim).transpose(0, 3, 2, 1, 4).reshape(n_micro, tokens, tp_size * heads * head_dim)
        attn = jnp.einsum('bsk,kh->bsh', o_rows, w_full.reshape(tp_size * heads * head_dim, hidden), preferred_element_type=jnp.float32)
        mid_rows = (act_in.astype(jnp.float32) + attn).astype(jnp.bfloat16)

        capacity = (4 * tokens) // experts
        slots = experts * capacity
        flat_ids = route_ids.reshape(n_micro, 2 * tokens)
        hits = (flat_ids[..., None] == jnp.arange(experts)).astype(jnp.bfloat16)
        before = (jnp.arange(2 * tokens)[:, None] > jnp.arange(2 * tokens)[None, :]).astype(jnp.bfloat16)
        rank = jnp.einsum('ij,bje->bie', before, hits, preferred_element_type=jnp.float32)
        slot_rank = jnp.sum(rank * hits.astype(jnp.float32), axis=-1).astype(jnp.int32)
        dest_slot = (flat_ids * capacity + slot_rank).reshape(n_micro, tokens, 2)
        slot_ix = jnp.arange(slots)
        pick0 = (dest_slot[:, :, 0:1] == slot_ix).astype(jnp.bfloat16)
        pick1 = (dest_slot[:, :, 1:2] == slot_ix).astype(jnp.bfloat16)
        send_buf = jnp.einsum('bts,bth->bsh', pick0 + pick1, mid_rows, preferred_element_type=jnp.float32).astype(jnp.bfloat16)
        recv_buf = lax.all_to_all(send_buf.reshape(n_micro, experts, capacity, hidden), ('cp', 'tp'), 1, 1, tiled=True)
        expert_in = recv_buf.reshape(n_micro, slots, hidden)
        gate_act = jnp.einsum('bth,hf->btf', expert_in, w_gate[0], preferred_element_type=jnp.float32)
        up_act = jnp.einsum('bth,hf->btf', expert_in, w_up[0], preferred_element_type=jnp.float32)
        mixed_act = (jax.nn.silu(gate_act) * up_act).astype(jnp.bfloat16)
        expert_out = jnp.einsum('btf,fh->bth', mixed_act, w_down[0], preferred_element_type=jnp.float32).astype(jnp.bfloat16)
        back = lax.all_to_all(expert_out.reshape(n_micro, experts, capacity, hidden), ('cp', 'tp'), 1, 1, tiled=True).reshape(n_micro, slots, hidden)
        z0 = jnp.einsum('bts,bsh->bth', pick0, back, preferred_element_type=jnp.float32)
        z1 = jnp.einsum('bts,bsh->bth', pick1, back, preferred_element_type=jnp.float32)
        combined = route_gates[:, :, 0:1] * z0 + route_gates[:, :, 1:2] * z1
        return (mid_rows.astype(jnp.float32) + combined).astype(jnp.bfloat16)

    return jax.shard_map(device_step, mesh=mesh, in_specs=(row_spec, row_spec, row_spec, head_spec, head_spec, head_spec, out_spec, expert_spec, expert_spec, expert_spec), out_specs=row_spec, check_vma=False)
```

```python
import functools

import jax
import jax.numpy as jnp
from jax import lax
from jax.experimental import pallas as pl
from jax.experimental.pallas import tpu as pltpu
from jax.sharding import PartitionSpec as P

LOG2E = 1.4426950408889634


def attention_body(pieces, piece_len, head_dim, qkv_ref, o_ref, s_ref):
    p = pl.program_id(0)
    half = pieces // 2
    factor = head_dim ** -0.5 * LOG2E

    def offset(n):
        return pl.multiple_of(jnp.where(n < half, 2 * piece_len * n, 2 * piece_len * (pieces - 1 - n) + piece_len), piece_len)

    q_rows = qkv_ref[pl.ds(offset(p), piece_len), 0:head_dim]

    def scores(n):
        k_rows = qkv_ref[pl.ds(offset(n), piece_len), head_dim:2 * head_dim]
        return lax.dot_general(q_rows, k_rows, (((1,), (1,)), ((), ())), preferred_element_type=jnp.float32)

    def fold(op, wide):
        parts = [wide[:, i * 128:(i + 1) * 128] for i in range(piece_len // 128)]
        while len(parts) > 1:
            parts = [op(a, b) for a, b in zip(parts[::2], parts[1::2])]
        return parts[0]

    def first(n, peak):
        s = scores(n)
        s_ref[n] = s
        return jnp.maximum(peak, fold(jnp.maximum, s))

    row = lax.broadcasted_iota(jnp.int32, (piece_len, piece_len), 0)
    col = lax.broadcasted_iota(jnp.int32, (piece_len, piece_len), 1)
    s_diag = jnp.where(col <= row, scores(p), -jnp.inf)
    s_ref[p] = s_diag
    peak = lax.fori_loop(0, p, first, fold(jnp.maximum, s_diag))
    peak = jnp.max(peak, axis=1, keepdims=True) * factor

    def second(n, carry):
        total, acc = carry
        e = jnp.exp2(s_ref[n] * factor - peak)
        v_rows = qkv_ref[pl.ds(offset(n), piece_len), 2 * head_dim:3 * head_dim]
        acc = acc + jnp.dot(e.astype(jnp.bfloat16), v_rows, preferred_element_type=jnp.float32)
        return total + fold(jnp.add, e), acc

    zero = jnp.zeros((piece_len, 128), jnp.float32)
    total, acc = lax.fori_loop(0, p + 1, second, (zero, jnp.zeros((piece_len, head_dim), jnp.float32)))
    total = jnp.sum(total, axis=1, keepdims=True)
    o_ref[pl.ds(offset(p), piece_len), :] = (acc / total).astype(jnp.bfloat16)


def attend_unit(qkv, pieces):
    rows, width = qkv.shape
    head_dim = width // 3
    piece_len = rows // pieces
    return pl.pallas_call(
        functools.partial(attention_body, pieces, piece_len, head_dim),
        grid=(pieces,),
        out_shape=jax.ShapeDtypeStruct((rows, head_dim), jnp.bfloat16),
        in_specs=[pl.BlockSpec((rows, width), lambda p: (0, 0))],
        out_specs=pl.BlockSpec((rows, head_dim), lambda p: (0, 0)),
        scratch_shapes=[pltpu.VMEM((pieces, piece_len, piece_len), jnp.float32)],
        compiler_params=pltpu.CompilerParams(vmem_limit_bytes=40 << 20),
        cost_estimate=pl.CostEstimate(flops=9 * 4 * rows * rows * head_dim // 16, bytes_accessed=4 * rows * head_dim * 2, transcendentals=0),
    )(qkv)


MESH_ID = pl.DeviceIdType.MESH


def expert_body(cp, tp, h_ref, sel_ref, pick_ref, g_ref, wg_hbm, wu_hbm, wd_hbm, y_ref,
                s0, s1, r0, r1, e0, e1, z0, z1, b0, b1, f0, f1, wg, wu, wd, rows_in, act, w_sem,
                out_x, out_y, mid_y, mid_x, ret_y, ret_x, fin_x, fin_y):
    d, c, t = lax.axis_index('data'), lax.axis_index('cp'), lax.axis_index('tp')
    cap, hidden = s0.shape[2], s0.shape[3]
    ff = wg.shape[1]
    nx = tp // 2
    ring = sorted(range(cp), key=lambda i: min(i, cp - i))
    x, k = t // 2, t % 2

    def tp_at(dx, dk):
        return ((x + dx) % nx) * 2 + (k + dk) % 2

    def tp_from(dx, dk):
        return ((x + nx - dx) % nx) * 2 + (k + dk) % 2

    def cp_at(dc):
        return (c + dc) % cp

    def cp_from(dc):
        return (c + cp - dc) % cp

    near = [(0, 1)] + [(dx, dk) for dx in ring[1:] for dk in (0, 1)]
    cols = ring[1:]

    weights = [pltpu.make_async_copy(a, b, w_sem.at[i]) for i, (a, b) in enumerate(((wg_hbm, wg), (wu_hbm, wu), (wd_hbm, wd)))]
    for copy in weights:
        copy.start()

    barrier = pltpu.get_barrier_semaphore()
    for dx, dk in near:
        pl.semaphore_signal(barrier, inc=1, device_id=(d, c, tp_at(dx, dk)), device_id_type=MESH_ID)
    for dc in cols:
        pl.semaphore_signal(barrier, inc=1, device_id=(d, cp_at(dc), t), device_id_type=MESH_ID)

    def send(src, dst, sems, key, cc, tt):
        return pltpu.make_async_remote_copy(src_ref=src, dst_ref=dst, send_sem=sems.at[(0,) + key], recv_sem=sems.at[(1,) + key], device_id=(d, cc, tt), device_id_type=MESH_ID)

    def select(b, buf):
        tile = 256

        @pl.loop(0, hidden // tile)
        def _(n):
            at = pl.ds(pl.multiple_of(n * tile, tile), tile)
            got = jnp.dot(sel_ref[b], h_ref[b, :, at], preferred_element_type=jnp.float32).astype(jnp.bfloat16)
            buf[:, :, :, at] = got.reshape(buf.shape[:3] + (tile,))

    select(0, s0)
    pl.semaphore_wait(barrier, len(near) + len(cols))
    first_x = {}
    for dx, dk in near:
        tt = tp_at(dx, dk)
        first_x[dx, dk] = send(s0.at[tt], r0.at[:, t], out_x, (dx, dk), c, tt)
        first_x[dx, dk].start()
    select(1, s1)
    first_y = {}
    for dc in cols:
        cc = cp_at(dc)
        first_y[dc] = send(s1.at[cc], r1.at[:, c], out_y, (dc,), cc, t)
        first_y[dc].start()
    r0[:, pl.ds(t, 1)] = s0[t][:, None]
    r1[:, pl.ds(c, 1)] = s1[c][:, None]

    for key in near:
        first_x[key].wait_recv()
    second_y = {}
    for dc in cols:
        cc = cp_at(dc)
        second_y[dc] = send(r0.at[cc], e0.at[c], mid_y, (dc,), cc, t)
        second_y[dc].start()
    for dc in cols:
        first_y[dc].wait_recv()
    second_x = {}
    for dx, dk in near:
        tt = tp_at(dx, dk)
        second_x[dx, dk] = send(r1.at[tt], e1.at[t], mid_x, (dx, dk), c, tt)
        second_x[dx, dk].start()
    for copy in weights:
        copy.wait()

    seg = tp * cap
    sub = cp * cap

    def run_expert():
        @pl.loop(0, ff // 128)
        def _(n):
            at = pl.ds(pl.multiple_of(n * 128, 128), 128)
            both = jnp.dot(rows_in[...], jnp.concatenate([wg[:, at], wu[:, at]], axis=1), preferred_element_type=jnp.float32)
            gate, up = both[:, :128], both[:, 128:]
            act[:, at] = (jax.nn.silu(gate) * up).astype(jnp.bfloat16)

        @pl.loop(0, hidden // 256)
        def _(n):
            at = pl.ds(pl.multiple_of(n * 256, 256), 256)
            rows_in[:, at] = jnp.dot(act[...], wd[:, at], preferred_element_type=jnp.float32).astype(jnp.bfloat16)

    back_y, back_x, last_x, last_y = {}, {}, {}, {}

    def forward(step):
        dc = dx = ring[step]
        if step:
            back_y[dc].wait_recv()
            back_x[dx, 0].wait_recv()
        back_x[dx, 1].wait_recv()
        ce = cp_at(dc)
        for tx, tk in near:
            tt = tp_at(tx, tk)
            last_x[dc, tx, tk] = send(b0.at[tt, ce], f0.at[t, ce], fin_x, (dc, tx, tk), c, tt)
            last_x[dc, tx, tk].start()
        pair = pl.ds(((x + dx) % nx) * 2, 2)
        for tc in cols:
            cc = cp_at(tc)
            last_y[dx, tc] = send(b1.at[cc, pair], f1.at[c, pair], fin_y, (dx, tc), cc, t)
            last_y[dx, tc].start()
        f0[t, pl.ds(ce, 1)] = b0[t, pl.ds(ce, 1)]
        f1[c, pair] = b1[c, pair]

    for step in range(cp):
        dc = dx = ring[step]
        if step == 0:
            second_x[0, 1].wait_recv()
            rows_in[0:seg] = r0[c].reshape(seg, hidden)
            rows_in[seg:seg + sub] = r1[t].reshape(sub, hidden)
            rows_in[seg + sub:seg + 2 * sub] = e1[tp_from(0, 1)].reshape(sub, hidden)
        else:
            second_y[dc].wait_recv()
            second_x[dx, 0].wait_recv()
            second_x[dx, 1].wait_recv()
            rows_in[0:seg] = e0[cp_from(dc)].reshape(seg, hidden)
            rows_in[seg:seg + sub] = e1[tp_from(dx, 0)].reshape(sub, hidden)
            rows_in[seg + sub:seg + 2 * sub] = e1[tp_from(dx, 1)].reshape(sub, hidden)
        run_expert()
        if step == 0:
            b0[:, pl.ds(c, 1)] = rows_in[0:seg].reshape(tp, 1, cap, hidden)
            b1[:, pl.ds(t, 1)] = rows_in[seg:seg + sub].reshape(cp, 1, cap, hidden)
        else:
            cs = cp_from(dc)
            z0[cs] = rows_in[0:seg].reshape(tp, cap, hidden)
            back_y[dc] = send(z0.at[cs], b0.at[:, c], ret_y, (dc,), cs, t)
            back_y[dc].start()
            ts = tp_from(dx, 0)
            z1[ts] = rows_in[seg:seg + sub].reshape(cp, cap, hidden)
            back_x[dx, 0] = send(z1.at[ts], b1.at[:, t], ret_x, (dx, 0), c, ts)
            back_x[dx, 0].start()
        ts = tp_from(dx, 1)
        z1[ts] = rows_in[seg + sub:seg + 2 * sub].reshape(cp, cap, hidden)
        back_x[dx, 1] = send(z1.at[ts], b1.at[:, t], ret_x, (dx, 1), c, ts)
        back_x[dx, 1].start()
        if step == 1:
            forward(0)
    for step in range(1, cp):
        forward(step)
    for copy in list(last_x.values()) + list(last_y.values()):
        copy.wait_recv()

    tokens = h_ref.shape[1]
    slots = cp * tp * cap

    @pl.loop(0, hidden // 256)
    def _(n):
        at = pl.ds(pl.multiple_of(n * 256, 256), 256)
        for b, buf in enumerate((f0, f1)):
            got = jnp.dot(pick_ref[b], buf[:, :, :, at].reshape(slots, 256), preferred_element_type=jnp.float32)
            mixed = g_ref[b, :, 0:1] * got[:tokens] + g_ref[b, :, 1:2] * got[tokens:]
            y_ref[b, :, at] = (h_ref[b, :, at].astype(jnp.float32) + mixed).astype(jnp.bfloat16)

    for group in (first_x, first_y, second_x, second_y, back_x, back_y, last_x, last_y):
        for copy in group.values():
            copy.wait_send()


def run_experts(mid_rows, sel, pick, route_gates, w_gate, w_up, w_down, cp, tp, cap):
    n_micro, tokens, hidden = mid_rows.shape
    ff = w_gate.shape[1]
    bf16 = jnp.bfloat16
    by_x, by_y = (tp, cp, cap, hidden), (cp, tp, cap, hidden)
    rows = 2 * (tp * cap)
    nx = tp // 2
    vmem = pl.BlockSpec(memory_space=pltpu.VMEM)
    any_spec = pl.BlockSpec(memory_space=pl.ANY)
    dma = pltpu.SemaphoreType.DMA
    return pl.pallas_call(
        functools.partial(expert_body, cp, tp),
        out_shape=jax.ShapeDtypeStruct(mid_rows.shape, bf16),
        in_specs=[vmem] * 4 + [any_spec] * 3,
        out_specs=vmem,
        scratch_shapes=[pltpu.VMEM(s, bf16) for s in (by_x, by_y, by_y, by_x, by_y, by_x, by_y, by_x, by_x, by_y, by_x, by_y)]
        + [pltpu.VMEM((hidden, ff), bf16), pltpu.VMEM((hidden, ff), bf16), pltpu.VMEM((ff, hidden), bf16)]
        + [pltpu.VMEM((rows, hidden), bf16), pltpu.VMEM((rows, ff), bf16)]
        + [dma((3,)), dma((2, nx, 2)), dma((2, cp)), dma((2, cp)), dma((2, nx, 2)), dma((2, cp)), dma((2, nx, 2)), dma((2, cp, nx, 2)), dma((2, nx, cp))],
        compiler_params=pltpu.CompilerParams(collective_id=1, has_side_effects=True, vmem_limit_bytes=60 << 20),
        cost_estimate=pl.CostEstimate(flops=6 * 4 * rows * hidden * ff, bytes_accessed=6 * hidden * ff, transcendentals=0),
    )(mid_rows, sel, pick, route_gates, w_gate, w_up, w_down)


def solution(mesh):
    cp_size = mesh.shape['cp']
    tp_size = mesh.shape['tp']
    experts = cp_size * tp_size
    row_spec = P(None, ('data', 'cp', 'tp'), None)
    head_spec = P(None, 'tp', None)
    out_spec = P('tp', None, None)
    expert_spec = P(('cp', 'tp'), None, None)

    def device_step(act_in, route_ids, route_gates, w_query, w_key, w_value, w_out, w_gate, w_up, w_down):
        n_micro, tokens, hidden = act_in.shape
        heads, head_dim = w_query.shape[1], w_query.shape[2]
        half_rows = tokens * tp_size
        w_qkv = jnp.concatenate([w_query, w_key, w_value], axis=2)
        x_half = lax.all_gather(act_in, 'tp', axis=1, tiled=True)
        w_full = lax.all_gather(w_out, 'tp', axis=0, tiled=True)
        qkv = jnp.einsum('bsh,hnd->bnsd', x_half, w_qkv, preferred_element_type=jnp.float32).astype(jnp.bfloat16)
        unit = lax.all_to_all(qkv.reshape(n_micro * heads, half_rows, 3 * head_dim), 'cp', 0, 0, tiled=True)
        o_unit = attend_unit(unit.reshape(cp_size * half_rows, 3 * head_dim), 2 * cp_size)
        o_recv = lax.all_to_all(o_unit.reshape(experts, tokens, head_dim), ('cp', 'tp'), 0, 0, tiled=True)
        o_rows = o_recv.reshape(n_micro, heads, tp_size, tokens, head_dim).transpose(0, 3, 2, 1, 4).reshape(n_micro, tokens, tp_size * heads * head_dim)
        attn = jnp.einsum('bsk,kh->bsh', o_rows, w_full.reshape(tp_size * heads * head_dim, hidden), preferred_element_type=jnp.float32)
        mid_rows = (act_in.astype(jnp.float32) + attn).astype(jnp.bfloat16)

        capacity = (4 * tokens) // experts
        slots = experts * capacity
        flat_ids = route_ids.reshape(n_micro, 2 * tokens)
        hits = (flat_ids[..., None] == jnp.arange(experts)).astype(jnp.bfloat16)
        before = (jnp.arange(2 * tokens)[:, None] > jnp.arange(2 * tokens)[None, :]).astype(jnp.bfloat16)
        rank = jnp.einsum('ij,bje->bie', before, hits, preferred_element_type=jnp.float32)
        slot_rank = jnp.sum(rank * hits.astype(jnp.float32), axis=-1).astype(jnp.int32)
        chip_slot = (flat_ids % tp_size * cp_size + flat_ids // tp_size) * capacity
        base_slot = jnp.where(jnp.arange(n_micro)[:, None] == 0, chip_slot, flat_ids * capacity)
        dest_slot = (base_slot + slot_rank).reshape(n_micro, tokens, 2).transpose(0, 2, 1).reshape(n_micro, 2 * tokens)
        slot_ix = jnp.arange(slots)
        pick = (dest_slot[:, :, None] == slot_ix).astype(jnp.bfloat16)
        sel = jnp.any((dest_slot[:, None, :] == slot_ix[:, None]).reshape(n_micro, slots, 2, tokens), axis=2).astype(jnp.bfloat16)
        return run_experts(mid_rows, sel, pick, route_gates, w_gate[0], w_up[0], w_down[0], cp_size, tp_size, capacity)

    return jax.shard_map(device_step, mesh=mesh, in_specs=(row_spec, row_spec, row_spec, head_spec, head_spec, head_spec, out_spec, expert_spec, expert_spec, expert_spec), out_specs=row_spec, check_vma=False)
```

```python
import functools

import jax
import jax.numpy as jnp
from jax import lax
from jax.experimental import pallas as pl
from jax.experimental.pallas import tpu as pltpu
from jax.sharding import PartitionSpec as P

LOG2E = 1.4426950408889634


MESH_ID = pl.DeviceIdType.MESH


def front_body(cp, tp, heads, x_hbm, w_hbm, wo_hbm, h_ref, xg, wo, w, u, q_out, s_ref, o_st, o_rows,
               in_sem, x_sem, wo_sem, u_sem, o_sem):
    d, c, t = lax.axis_index('data'), lax.axis_index('cp'), lax.axis_index('tp')
    nx = tp // 2
    x, k = t // 2, t % 2
    tokens, hidden = x_hbm.shape[1], x_hbm.shape[2]
    half_rows = tokens * tp
    pieces = 2 * cp
    piece_len = half_rows // 2
    head_dim = o_st.shape[1]
    width = 3 * head_dim
    left, right, far = ((x + nx - 1) % nx) * 2, ((x + 1) % nx) * 2, ((x + 2) % nx) * 2
    mine, other = k, 1 - k
    mate = 2 * x + other

    loads = [pltpu.make_async_copy(x_hbm, xg.at[t], in_sem.at[0]), pltpu.make_async_copy(w_hbm, w, in_sem.at[1]), pltpu.make_async_copy(wo_hbm, wo.at[t], in_sem.at[2])]
    for load in loads:
        load.start()
    barrier = pltpu.get_barrier_semaphore()
    peers = [(dc, dt) for dc in range(cp) for dt in range(tp) if dc or dt]
    for dc, dt in peers:
        pl.semaphore_signal(barrier, inc=1, device_id=(d, (c + dc) % cp, (t + dt) % tp), device_id_type=MESH_ID)
    pl.semaphore_wait(barrier, len(peers))

    def send(src, dst, sems, key, cc, tt):
        return pltpu.make_async_remote_copy(src_ref=src, dst_ref=dst, send_sem=sems.at[(0,) + key], recv_sem=sems.at[(1,) + key], device_id=(d, cc, tt), device_id_type=MESH_ID)

    names = ['r0', 'r1', 'r2', 'l0', 'l1', 'l2'] + ['p%d' % i for i in range(8)]

    def ring(buf, sems):
        sent = {}

        def start(name, src, part, target):
            sent[name] = send(buf.at[src, part], buf.at[src, part], sems, (names.index(name),), c, target)
            sent[name].start()

        def wave(n):
            if n == 0:
                start('p0', t, 0, mate)
                start('p1', t, 1, mate)
                start('r0', t, 0, right + mine)
                start('l0', t, 1, left + mine)
                start('r1', t, 1, right + mine)
                start('l1', t, 0, left + mine)
            elif n == 1:
                sent['r0'].wait_recv()
                start('r2', left + mine, 0, right + mine)
                start('p2', left + mine, 0, mate)
                sent['l0'].wait_recv()
                start('l2', right + mine, 1, left + mine)
                start('p3', right + mine, 1, mate)
            elif n == 2:
                sent['r1'].wait_recv()
                start('p4', left + mine, 1, mate)
                sent['l1'].wait_recv()
                start('p5', right + mine, 0, mate)
            else:
                sent['r2'].wait_recv()
                start('p6', far + mine, 0, mate)
                sent['l2'].wait_recv()
                start('p7', far + mine, 1, mate)
        return sent, wave

    x_sent, x_wave = ring(xg, x_sem)
    wo_sent, wo_wave = ring(wo, wo_sem)
    u_sent = {}

    def project(tt, s):
        @pl.loop(0, heads * width // 256)
        def _(n):
            at = pl.ds(pl.multiple_of(n * 256, 256), 256)
            q_out[tt, s, :, at] = jnp.dot(xg[tt, s], w[:, at], preferred_element_type=jnp.float32).astype(jnp.bfloat16)

        rows = pl.ds(pl.multiple_of(c * half_rows + tt * tokens, tokens), tokens)
        for dc in (1, cp - 1, 2):
            c2 = (c + dc) % cp
            lanes = pl.ds(pl.multiple_of(c2 % heads * width, 128), width)
            copy = send(q_out.at[tt, s, :, lanes], u.at[rows], u_sem, (dc, tt), c2, t)
            pl.when(c2 // heads == s)(copy.start)
            u_sent.setdefault(dc, []).append(copy)

        @pl.when(c // heads == s)
        def _():
            lanes = pl.ds(pl.multiple_of(c % heads * width, 128), width)
            u[rows] = q_out[tt, s, :, lanes]

    loads[0].wait()
    x_wave(0)
    loads[1].wait()
    project(t, 0)
    project(t, 1)
    for s, name in ((0, 'p0'), (1, 'p1')):
        x_sent[name].wait_recv()
        project(mate, s)
    x_wave(1)
    loads[2].wait()
    wo_wave(0)
    project(left + mine, 0)
    project(right + mine, 1)
    x_sent['p2'].wait_recv()
    project(left + other, 0)
    x_sent['p3'].wait_recv()
    project(right + other, 1)
    x_wave(2)
    project(left + mine, 1)
    project(right + mine, 0)
    x_sent['p4'].wait_recv()
    project(left + other, 1)
    x_sent['p5'].wait_recv()
    project(right + other, 0)
    x_wave(3)
    project(far + mine, 0)
    project(far + mine, 1)
    x_sent['p6'].wait_recv()
    project(far + other, 0)
    x_sent['p7'].wait_recv()
    project(far + other, 1)

    def u_copy(dc, tt):
        c2 = (c + dc) % cp
        lanes = pl.ds(pl.multiple_of(c2 % heads * width, 128), width)
        rows = pl.ds(pl.multiple_of(c * half_rows + tt * tokens, tokens), tokens)
        return send(q_out.at[tt, c2 // heads, :, lanes], u.at[rows], u_sem, (dc, tt), c2, t)

    for dc in (1, cp - 1, 2):
        for tt in range(tp):
            u_copy(dc, tt).wait_recv()
    wo_wave(1)

    factor = head_dim ** -0.5 * LOG2E
    per_half = tp // 2

    def offset(n):
        return pl.multiple_of(jnp.where(n < cp, 2 * piece_len * n, 2 * piece_len * (pieces - 1 - n) + piece_len), piece_len)

    def fold(op, wide):
        parts = [wide[:, i * 128:(i + 1) * 128] for i in range(piece_len // 128)]
        while len(parts) > 1:
            parts = [op(a, b) for a, b in zip(parts[::2], parts[1::2])]
        return parts[0]

    row = lax.broadcasted_iota(jnp.int32, (piece_len, piece_len), 0)
    col = lax.broadcasted_iota(jnp.int32, (piece_len, piece_len), 1)
    unit_seq = c // heads
    unit_head = t * heads + c % heads

    def o_copy(rows, dcl, dtl, cc, tt):
        lanes = pl.ds(pl.multiple_of(unit_head * head_dim, 128), head_dim)
        return send(o_st.at[rows], o_rows.at[unit_seq, :, lanes], o_sem, (dcl, dtl), cc, tt)

    @pl.loop(0, pieces)
    def _(p):
        q_rows = u[pl.ds(offset(p), piece_len), 0:head_dim]

        def scores(n):
            k_rows = u[pl.ds(offset(n), piece_len), head_dim:2 * head_dim]
            return lax.dot_general(q_rows, k_rows, (((1,), (1,)), ((), ())), preferred_element_type=jnp.float32)

        def first(n, peak):
            s = scores(n)
            s_ref[n] = s
            return jnp.maximum(peak, fold(jnp.maximum, s))

        s_diag = jnp.where(col <= row, scores(p), -jnp.inf)
        s_ref[p] = s_diag
        peak = lax.fori_loop(0, p, first, fold(jnp.maximum, s_diag))
        peak = jnp.max(peak, axis=1, keepdims=True) * factor

        def second(n, carry):
            total, acc = carry
            e = jnp.exp2(s_ref[n] * factor - peak)
            v_rows = u[pl.ds(offset(n), piece_len), 2 * head_dim:3 * head_dim]
            acc = acc + jnp.dot(e.astype(jnp.bfloat16), v_rows, preferred_element_type=jnp.float32)
            return total + fold(jnp.add, e), acc

        total, acc = lax.fori_loop(0, p + 1, second, (jnp.zeros((piece_len, 128), jnp.float32), jnp.zeros((piece_len, head_dim), jnp.float32)))
        total = jnp.sum(total, axis=1, keepdims=True)
        o_st[pl.ds(offset(p), piece_len), :] = (acc / total).astype(jnp.bfloat16)
        low = p < cp
        cc = jnp.where(low, p, pieces - 1 - p)
        for i in range(per_half):
            tt = jnp.where(low, i, per_half + i)
            rows = pl.ds(pl.multiple_of(offset(p) + i * tokens, tokens), tokens)
            dcl, dtl = (cc - c + cp) % cp, (tt - t + tp) % tp
            pl.when(dcl + dtl > 0)(o_copy(rows, dcl, dtl, cc, tt).start)

            @pl.when(dcl + dtl == 0)
            def _():
                lanes = pl.ds(pl.multiple_of(unit_head * head_dim, 128), head_dim)
                o_rows[unit_seq, :, lanes] = o_st[rows]

    wo_wave(2)
    wo_wave(3)
    for i in range(8):
        wo_sent['p%d' % i].wait_recv()
    first_rows = pl.ds(0, tokens)
    o_all = [o_copy(first_rows, dc, dt, (c + dc) % cp, (t + dt) % tp) for dc, dt in peers]
    for copy in o_all:
        copy.wait_recv()

    full = tp * heads * head_dim

    @pl.loop(0, hidden // 256)
    def _(n):
        at = pl.ds(pl.multiple_of(n * 256, 256), 256)
        a = jnp.dot(o_rows[...].reshape(2 * tokens, full), wo[:, :, :, at].reshape(full, 256), preferred_element_type=jnp.float32)
        h_ref[:, :, at] = (xg[t, :, :, at].astype(jnp.float32) + a.reshape(2, tokens, 256)).astype(jnp.bfloat16)

    for copy in list(x_sent.values()) + list(wo_sent.values()) + o_all:
        copy.wait_send()
    for dc in (1, cp - 1, 2):
        for tt in range(tp):
            u_copy(dc, tt).wait_send()


def run_front(act_in, w_qkv, w_out, cp, tp, heads):
    n_micro, tokens, hidden = act_in.shape
    head_dim = w_out.shape[1]
    half_rows = tokens * tp
    rows = cp * half_rows
    bf16 = jnp.bfloat16
    any_spec = pl.BlockSpec(memory_space=pl.ANY)
    dma = pltpu.SemaphoreType.DMA
    vmem = [(tp, n_micro, tokens, hidden), (tp, heads, head_dim, hidden), (hidden, heads * 3 * head_dim), (rows, 3 * head_dim), (tp, n_micro, tokens, heads * 3 * head_dim)]
    piece = half_rows // 2
    return pl.pallas_call(
        functools.partial(front_body, cp, tp, heads),
        out_shape=jax.ShapeDtypeStruct(act_in.shape, bf16),
        in_specs=[any_spec] * 3,
        out_specs=pl.BlockSpec(memory_space=pltpu.VMEM),
        scratch_shapes=[pltpu.VMEM(s, bf16) for s in vmem]
        + [pltpu.VMEM((2 * cp, piece, piece), jnp.float32), pltpu.VMEM((rows, head_dim), bf16), pltpu.VMEM((n_micro, tokens, tp * heads * head_dim), bf16)]
        + [dma((3,)), dma((2, 14)), dma((2, 14)), dma((2, cp, tp)), dma((2, cp, tp))],
        compiler_params=pltpu.CompilerParams(collective_id=2, has_side_effects=True, vmem_limit_bytes=56 << 20),
        cost_estimate=pl.CostEstimate(flops=8 * rows * hidden * head_dim * 3, bytes_accessed=20 << 20, transcendentals=0),
    )(act_in, w_qkv, w_out)


def expert_body(cp, tp, h_ref, sel_ref, pick_ref, g_ref, wg_hbm, wu_hbm, wd_hbm, y_ref,
                s0, s1, r0, r1, e0, e1, z0, z1, b0, b1, f0, f1, wg, wu, wd, rows_in, act, w_sem,
                out_x, out_y, mid_y, mid_x, ret_y, ret_x, fin_x, fin_y):
    d, c, t = lax.axis_index('data'), lax.axis_index('cp'), lax.axis_index('tp')
    cap, hidden = s0.shape[2], s0.shape[3]
    ff = wg.shape[1]
    nx = tp // 2
    ring = sorted(range(cp), key=lambda i: min(i, cp - i))
    x, k = t // 2, t % 2

    def tp_at(dx, dk):
        return ((x + dx) % nx) * 2 + (k + dk) % 2

    def tp_from(dx, dk):
        return ((x + nx - dx) % nx) * 2 + (k + dk) % 2

    def cp_at(dc):
        return (c + dc) % cp

    def cp_from(dc):
        return (c + cp - dc) % cp

    near = [(0, 1)] + [(dx, dk) for dx in ring[1:] for dk in (0, 1)]
    cols = ring[1:]

    weights = [pltpu.make_async_copy(a, b, w_sem.at[i]) for i, (a, b) in enumerate(((wg_hbm, wg), (wu_hbm, wu), (wd_hbm, wd)))]
    for copy in weights:
        copy.start()

    barrier = pltpu.get_barrier_semaphore()
    for dx, dk in near:
        pl.semaphore_signal(barrier, inc=1, device_id=(d, c, tp_at(dx, dk)), device_id_type=MESH_ID)
    for dc in cols:
        pl.semaphore_signal(barrier, inc=1, device_id=(d, cp_at(dc), t), device_id_type=MESH_ID)

    def send(src, dst, sems, key, cc, tt):
        return pltpu.make_async_remote_copy(src_ref=src, dst_ref=dst, send_sem=sems.at[(0,) + key], recv_sem=sems.at[(1,) + key], device_id=(d, cc, tt), device_id_type=MESH_ID)

    def select(b, buf):
        tile = 256

        @pl.loop(0, hidden // tile)
        def _(n):
            at = pl.ds(pl.multiple_of(n * tile, tile), tile)
            got = jnp.dot(sel_ref[b], h_ref[b, :, at], preferred_element_type=jnp.float32).astype(jnp.bfloat16)
            buf[:, :, :, at] = got.reshape(buf.shape[:3] + (tile,))

    select(0, s0)
    pl.semaphore_wait(barrier, len(near) + len(cols))
    first_x = {}
    for dx, dk in near:
        tt = tp_at(dx, dk)
        first_x[dx, dk] = send(s0.at[tt], r0.at[:, t], out_x, (dx, dk), c, tt)
        first_x[dx, dk].start()
    select(1, s1)
    first_y = {}
    for dc in cols:
        cc = cp_at(dc)
        first_y[dc] = send(s1.at[cc], r1.at[:, c], out_y, (dc,), cc, t)
        first_y[dc].start()
    r0[:, pl.ds(t, 1)] = s0[t][:, None]
    r1[:, pl.ds(c, 1)] = s1[c][:, None]

    for key in near:
        first_x[key].wait_recv()
    second_y = {}
    for dc in cols:
        cc = cp_at(dc)
        second_y[dc] = send(r0.at[cc], e0.at[c], mid_y, (dc,), cc, t)
        second_y[dc].start()
    for dc in cols:
        first_y[dc].wait_recv()
    second_x = {}
    for dx, dk in near:
        tt = tp_at(dx, dk)
        second_x[dx, dk] = send(r1.at[tt], e1.at[t], mid_x, (dx, dk), c, tt)
        second_x[dx, dk].start()
    for copy in weights:
        copy.wait()

    seg = tp * cap
    sub = cp * cap

    def run_expert():
        @pl.loop(0, ff // 128)
        def _(n):
            at = pl.ds(pl.multiple_of(n * 128, 128), 128)
            both = jnp.dot(rows_in[...], jnp.concatenate([wg[:, at], wu[:, at]], axis=1), preferred_element_type=jnp.float32)
            gate, up = both[:, :128], both[:, 128:]
            act[:, at] = (jax.nn.silu(gate) * up).astype(jnp.bfloat16)

        @pl.loop(0, hidden // 256)
        def _(n):
            at = pl.ds(pl.multiple_of(n * 256, 256), 256)
            rows_in[:, at] = jnp.dot(act[...], wd[:, at], preferred_element_type=jnp.float32).astype(jnp.bfloat16)

    back_y, back_x, last_x, last_y = {}, {}, {}, {}

    def forward(step):
        dc = dx = ring[step]
        if step:
            back_y[dc].wait_recv()
            back_x[dx, 0].wait_recv()
        back_x[dx, 1].wait_recv()
        ce = cp_at(dc)
        for tx, tk in near:
            tt = tp_at(tx, tk)
            last_x[dc, tx, tk] = send(b0.at[tt, ce], f0.at[t, ce], fin_x, (dc, tx, tk), c, tt)
            last_x[dc, tx, tk].start()
        pair = pl.ds(((x + dx) % nx) * 2, 2)
        for tc in cols:
            cc = cp_at(tc)
            last_y[dx, tc] = send(b1.at[cc, pair], f1.at[c, pair], fin_y, (dx, tc), cc, t)
            last_y[dx, tc].start()
        f0[t, pl.ds(ce, 1)] = b0[t, pl.ds(ce, 1)]
        f1[c, pair] = b1[c, pair]

    for step in range(cp):
        dc = dx = ring[step]
        if step == 0:
            second_x[0, 1].wait_recv()
            rows_in[0:seg] = r0[c].reshape(seg, hidden)
            rows_in[seg:seg + sub] = r1[t].reshape(sub, hidden)
            rows_in[seg + sub:seg + 2 * sub] = e1[tp_from(0, 1)].reshape(sub, hidden)
        else:
            second_y[dc].wait_recv()
            second_x[dx, 0].wait_recv()
            second_x[dx, 1].wait_recv()
            rows_in[0:seg] = e0[cp_from(dc)].reshape(seg, hidden)
            rows_in[seg:seg + sub] = e1[tp_from(dx, 0)].reshape(sub, hidden)
            rows_in[seg + sub:seg + 2 * sub] = e1[tp_from(dx, 1)].reshape(sub, hidden)
        run_expert()
        if step == 0:
            b0[:, pl.ds(c, 1)] = rows_in[0:seg].reshape(tp, 1, cap, hidden)
            b1[:, pl.ds(t, 1)] = rows_in[seg:seg + sub].reshape(cp, 1, cap, hidden)
        else:
            cs = cp_from(dc)
            z0[cs] = rows_in[0:seg].reshape(tp, cap, hidden)
            back_y[dc] = send(z0.at[cs], b0.at[:, c], ret_y, (dc,), cs, t)
            back_y[dc].start()
            ts = tp_from(dx, 0)
            z1[ts] = rows_in[seg:seg + sub].reshape(cp, cap, hidden)
            back_x[dx, 0] = send(z1.at[ts], b1.at[:, t], ret_x, (dx, 0), c, ts)
            back_x[dx, 0].start()
        ts = tp_from(dx, 1)
        z1[ts] = rows_in[seg + sub:seg + 2 * sub].reshape(cp, cap, hidden)
        back_x[dx, 1] = send(z1.at[ts], b1.at[:, t], ret_x, (dx, 1), c, ts)
        back_x[dx, 1].start()
        if step == 1:
            forward(0)
    for step in range(1, cp):
        forward(step)
    for copy in list(last_x.values()) + list(last_y.values()):
        copy.wait_recv()

    tokens = h_ref.shape[1]
    slots = cp * tp * cap

    @pl.loop(0, hidden // 256)
    def _(n):
        at = pl.ds(pl.multiple_of(n * 256, 256), 256)
        for b, buf in enumerate((f0, f1)):
            got = jnp.dot(pick_ref[b], buf[:, :, :, at].reshape(slots, 256), preferred_element_type=jnp.float32)
            mixed = g_ref[b, :, 0:1] * got[:tokens] + g_ref[b, :, 1:2] * got[tokens:]
            y_ref[b, :, at] = (h_ref[b, :, at].astype(jnp.float32) + mixed).astype(jnp.bfloat16)

    for group in (first_x, first_y, second_x, second_y, back_x, back_y, last_x, last_y):
        for copy in group.values():
            copy.wait_send()


def run_experts(mid_rows, sel, pick, route_gates, w_gate, w_up, w_down, cp, tp, cap):
    n_micro, tokens, hidden = mid_rows.shape
    ff = w_gate.shape[1]
    bf16 = jnp.bfloat16
    by_x, by_y = (tp, cp, cap, hidden), (cp, tp, cap, hidden)
    rows = 2 * (tp * cap)
    nx = tp // 2
    vmem = pl.BlockSpec(memory_space=pltpu.VMEM)
    any_spec = pl.BlockSpec(memory_space=pl.ANY)
    dma = pltpu.SemaphoreType.DMA
    return pl.pallas_call(
        functools.partial(expert_body, cp, tp),
        out_shape=jax.ShapeDtypeStruct(mid_rows.shape, bf16),
        in_specs=[vmem] * 4 + [any_spec] * 3,
        out_specs=vmem,
        scratch_shapes=[pltpu.VMEM(s, bf16) for s in (by_x, by_y, by_y, by_x, by_y, by_x, by_y, by_x, by_x, by_y, by_x, by_y)]
        + [pltpu.VMEM((hidden, ff), bf16), pltpu.VMEM((hidden, ff), bf16), pltpu.VMEM((ff, hidden), bf16)]
        + [pltpu.VMEM((rows, hidden), bf16), pltpu.VMEM((rows, ff), bf16)]
        + [dma((3,)), dma((2, nx, 2)), dma((2, cp)), dma((2, cp)), dma((2, nx, 2)), dma((2, cp)), dma((2, nx, 2)), dma((2, cp, nx, 2)), dma((2, nx, cp))],
        compiler_params=pltpu.CompilerParams(collective_id=1, has_side_effects=True, vmem_limit_bytes=60 << 20),
        cost_estimate=pl.CostEstimate(flops=6 * 4 * rows * hidden * ff, bytes_accessed=6 * hidden * ff, transcendentals=0),
    )(mid_rows, sel, pick, route_gates, w_gate, w_up, w_down)


def solution(mesh):
    cp_size = mesh.shape['cp']
    tp_size = mesh.shape['tp']
    experts = cp_size * tp_size
    row_spec = P(None, ('data', 'cp', 'tp'), None)
    head_spec = P(None, 'tp', None)
    out_spec = P('tp', None, None)
    expert_spec = P(('cp', 'tp'), None, None)

    def device_step(act_in, route_ids, route_gates, w_query, w_key, w_value, w_out, w_gate, w_up, w_down):
        n_micro, tokens, hidden = act_in.shape
        heads, head_dim = w_query.shape[1], w_query.shape[2]
        w_qkv = jnp.concatenate([w_query, w_key, w_value], axis=2).reshape(hidden, heads * 3 * head_dim)
        mid_rows = run_front(act_in, w_qkv, w_out, cp_size, tp_size, heads)

        capacity = (4 * tokens) // experts
        slots = experts * capacity
        flat_ids = route_ids.reshape(n_micro, 2 * tokens)
        hits = (flat_ids[..., None] == jnp.arange(experts)).astype(jnp.bfloat16)
        before = (jnp.arange(2 * tokens)[:, None] > jnp.arange(2 * tokens)[None, :]).astype(jnp.bfloat16)
        rank = jnp.einsum('ij,bje->bie', before, hits, preferred_element_type=jnp.float32)
        slot_rank = jnp.sum(rank * hits.astype(jnp.float32), axis=-1).astype(jnp.int32)
        chip_slot = (flat_ids % tp_size * cp_size + flat_ids // tp_size) * capacity
        base_slot = jnp.where(jnp.arange(n_micro)[:, None] == 0, chip_slot, flat_ids * capacity)
        dest_slot = (base_slot + slot_rank).reshape(n_micro, tokens, 2).transpose(0, 2, 1).reshape(n_micro, 2 * tokens)
        slot_ix = jnp.arange(slots)
        pick = (dest_slot[:, :, None] == slot_ix).astype(jnp.bfloat16)
        sel = jnp.any((dest_slot[:, None, :] == slot_ix[:, None]).reshape(n_micro, slots, 2, tokens), axis=2).astype(jnp.bfloat16)
        return run_experts(mid_rows, sel, pick, route_gates, w_gate[0], w_up[0], w_down[0], cp_size, tp_size, capacity)

    return jax.shard_map(device_step, mesh=mesh, in_specs=(row_spec, row_spec, row_spec, head_spec, head_spec, head_spec, out_spec, expert_spec, expert_spec, expert_spec), out_specs=row_spec, check_vma=False)
```

```python
import functools

import jax
import jax.numpy as jnp
from jax import lax
from jax.experimental import pallas as pl
from jax.experimental.pallas import tpu as pltpu
from jax.sharding import PartitionSpec as P

LOG2E = 1.4426950408889634


MESH_ID = pl.DeviceIdType.MESH


def front_body(cp, tp, heads, x_hbm, wq_hbm, wk_hbm, wv_hbm, wo_hbm, h_ref, xg, wo, w, u, q_out, s_ref, o_st, o_rows,
               peaks, totals, accs, raw, in_sem, x_sem, bulk_sem, strip_sem, lane_sem, mate_sem, u_sem, o_sem):
    d, c, t = lax.axis_index('data'), lax.axis_index('cp'), lax.axis_index('tp')
    nx = tp // 2
    x, k = t // 2, t % 2
    tokens, hidden = x_hbm.shape[1], x_hbm.shape[2]
    half_rows = tokens * tp
    pieces = 2 * cp
    piece_len = half_rows // 2
    head_dim = o_st.shape[1]
    width = 3 * head_dim
    left, right, far = ((x + nx - 1) % nx) * 2, ((x + 1) % nx) * 2, ((x + 2) % nx) * 2
    mine, other = k, 1 - k
    mate = 2 * x + other

    split = wo_hbm.shape[0] - 16 * cp
    strip_rows = pl.ds(split + 16 * c, 16)
    loads = [pltpu.make_async_copy(x_hbm, xg.at[t], in_sem.at[0]), pltpu.make_async_copy(wq_hbm, raw.at[0], in_sem.at[1]), pltpu.make_async_copy(wo_hbm.at[pl.ds(0, split)], wo.at[x, k, pl.ds(0, split)], in_sem.at[2]),
             pltpu.make_async_copy(wo_hbm.at[strip_rows], wo.at[x, k, strip_rows], in_sem.at[3]),
             pltpu.make_async_copy(wk_hbm, raw.at[1], in_sem.at[4]), pltpu.make_async_copy(wv_hbm, raw.at[2], in_sem.at[5])]
    for load in loads:
        load.start()
    barrier = pltpu.get_barrier_semaphore()
    peers = [(dc, dt) for dc in range(cp) for dt in range(tp) if dc or dt]
    for dc, dt in peers:
        pl.semaphore_signal(barrier, inc=1, device_id=(d, (c + dc) % cp, (t + dt) % tp), device_id_type=MESH_ID)
    pl.semaphore_wait(barrier, len(peers))

    def send(src, dst, sems, key, cc, tt):
        return pltpu.make_async_remote_copy(src_ref=src, dst_ref=dst, send_sem=sems.at[(0,) + key], recv_sem=sems.at[(1,) + key], device_id=(d, cc, tt), device_id_type=MESH_ID)

    names = ['r0', 'r1', 'r2', 'l0', 'l1', 'l2'] + ['p%d' % i for i in range(8)]

    def ring(view, sems, with_mate):
        sent = {}

        def start(name, src, part, target):
            if with_mate or name[0] != 'p':
                sent[name] = send(view(src, part), view(src, part), sems, (names.index(name),), c, target)
                sent[name].start()

        def wave(n):
            if n == 0:
                start('p0', t, 0, mate)
                start('p1', t, 1, mate)
                start('r0', t, 0, right + mine)
                start('l0', t, 1, left + mine)
                start('r1', t, 1, right + mine)
                start('l1', t, 0, left + mine)
            elif n == 1:
                sent['r0'].wait_recv()
                start('r2', left + mine, 0, right + mine)
                start('p2', left + mine, 0, mate)
                sent['l0'].wait_recv()
                start('l2', right + mine, 1, left + mine)
                start('p3', right + mine, 1, mate)
            elif n == 2:
                sent['r1'].wait_recv()
                start('p4', left + mine, 1, mate)
                sent['l1'].wait_recv()
                start('p5', right + mine, 0, mate)
            else:
                sent['r2'].wait_recv()
                start('p6', far + mine, 0, mate)
                sent['l2'].wait_recv()
                start('p7', far + mine, 1, mate)
        return sent, wave

    part_rows = split // 2

    def bulk(src, part):
        return wo.at[src // 2, src % 2, pl.ds(part * part_rows, part_rows)]

    def strip(src, part):
        return wo.at[src // 2, src % 2, pl.ds(split + 16 * c, 16), pl.ds(part * (hidden // 2), hidden // 2)]

    def lane(q):
        return wo.at[:, k, pl.ds(split + 16 * q, 16)]

    x_sent, x_wave = ring(lambda src, part: xg.at[src, part], x_sem, True)
    bulk_sent, bulk_wave = ring(bulk, bulk_sem, True)
    strip_sent, strip_wave = ring(strip, strip_sem, False)
    lane_y = {dc: send(lane(c), lane(c), lane_sem, (dc,), (c + dc) % cp, t) for dc in (1, cp - 1, 2)}
    lane_mate = {dc: send(lane((c + cp - dc) % cp), lane((c + cp - dc) % cp), mate_sem, (dc,), c, mate) for dc in (0, 1, cp - 1, 2)}

    def project(tt, s):
        @pl.loop(0, heads * width // 256)
        def _(n):
            at = pl.ds(pl.multiple_of(n * 256, 256), 256)
            q_out[tt, s, :, at] = jnp.dot(xg[tt, s], w[:, at], preferred_element_type=jnp.float32).astype(jnp.bfloat16)

        rows = pl.ds(pl.multiple_of(c * half_rows + tt * tokens, tokens), tokens)
        for dc in (1, cp - 1, 2):
            c2 = (c + dc) % cp
            lanes = pl.ds(pl.multiple_of(c2 % heads * width, 128), width)
            copy = send(q_out.at[tt, s, :, lanes], u.at[rows], u_sem, (dc, tt), c2, t)
            pl.when(c2 // heads == s)(copy.start)

        @pl.when(c // heads == s)
        def _():
            lanes = pl.ds(pl.multiple_of(c % heads * width, 128), width)
            u[rows] = q_out[tt, s, :, lanes]

    loads[0].wait()
    x_wave(0)
    loads[3].wait()
    strip_wave(0)
    for i in (1, 4, 5):
        loads[i].wait()

    @pl.loop(0, hidden // 32)
    def _(i):
        at = pl.ds(pl.multiple_of(i * 32, 32), 32)
        for j in range(3):
            flat = raw[j, at].reshape(32, heads * head_dim)
            for n in range(heads):
                w[at, n * width + j * head_dim:n * width + (j + 1) * head_dim] = flat[:, n * head_dim:(n + 1) * head_dim]

    project(t, 0)
    project(t, 1)
    for s, name in ((0, 'p0'), (1, 'p1')):
        x_sent[name].wait_recv()
        project(mate, s)
    x_wave(1)
    project(left + mine, 0)
    project(right + mine, 1)
    x_sent['p2'].wait_recv()
    project(left + other, 0)
    x_sent['p3'].wait_recv()
    project(right + other, 1)
    x_wave(2)
    strip_wave(1)
    loads[2].wait()
    bulk_wave(0)
    project(left + mine, 1)
    project(right + mine, 0)
    x_sent['p4'].wait_recv()
    project(left + other, 1)
    x_sent['p5'].wait_recv()
    project(right + other, 0)
    x_wave(3)
    project(far + mine, 0)
    project(far + mine, 1)
    x_sent['p6'].wait_recv()
    project(far + other, 0)
    x_sent['p7'].wait_recv()
    project(far + other, 1)
    strip_wave(2)
    strip_wave(3)
    for dc in (1, cp - 1, 2):
        lane_y[dc].start()
    lane_mate[0].start()

    def u_copy(dc, tt):
        c2 = (c + dc) % cp
        lanes = pl.ds(pl.multiple_of(c2 % heads * width, 128), width)
        rows = pl.ds(pl.multiple_of(c * half_rows + tt * tokens, tokens), tokens)
        return send(q_out.at[tt, c2 // heads, :, lanes], u.at[rows], u_sem, (dc, tt), c2, t)

    for dc in (1, cp - 1, 2):
        for tt in range(tp):
            u_copy(dc, tt).wait_recv()
    bulk_wave(1)

    factor = head_dim ** -0.5 * LOG2E
    per_half = tp // 2

    def offset(n):
        return pl.multiple_of(jnp.where(n < cp, 2 * piece_len * n, 2 * piece_len * (pieces - 1 - n) + piece_len), piece_len)

    def fold(op, wide):
        parts = [wide[:, i * 128:(i + 1) * 128] for i in range(piece_len // 128)]
        while len(parts) > 1:
            parts = [op(a, b) for a, b in zip(parts[::2], parts[1::2])]
        return parts[0]

    row = lax.broadcasted_iota(jnp.int32, (piece_len, piece_len), 0)
    col = lax.broadcasted_iota(jnp.int32, (piece_len, piece_len), 1)
    unit_seq = c // heads
    unit_head = t * heads + c % heads

    def o_copy(rows, dcl, dtl, cc, tt):
        lanes = pl.ds(pl.multiple_of(unit_head * head_dim, 128), head_dim)
        return send(o_st.at[rows], o_rows.at[unit_seq, :, lanes], o_sem, (dcl, dtl), cc, tt)

    gap = col - row

    @pl.loop(0, cp)
    def _(p):
        lo, hi = p, pieces - 1 - p

        def place(j):
            if j >= cp:
                return hi, j - p - 1, 1
            is_lo = j <= p
            return jnp.where(is_lo, lo, hi), jnp.where(is_lo, j, j - p - 1), jnp.where(is_lo, 0, 1)

        def scores(j):
            piece, n, _ = place(j)
            q_rows = u[pl.ds(offset(piece), piece_len), 0:head_dim]
            k_rows = u[pl.ds(offset(n), piece_len), head_dim:2 * head_dim]
            s = lax.dot_general(q_rows, k_rows, (((1,), (1,)), ((), ())), preferred_element_type=jnp.float32)
            if j == pieces:
                s = jnp.where(gap <= 0, s, -jnp.inf)
            elif j < cp:
                s = jnp.where(gap <= jnp.where(j == p, 0, piece_len), s, -jnp.inf)
            s_ref[j] = s
            return fold(jnp.maximum, s)

        high = scores(cp)
        for j in range(cp + 1, pieces + 1):
            high = jnp.maximum(high, scores(j))
        peaks[1] = high
        peaks[0] = jnp.full_like(high, -jnp.inf)
        for j in range(cp):
            slot = place(j)[2]
            peaks[slot] = jnp.maximum(peaks[slot], scores(j))
        for slot in range(2):
            peaks[slot] = jnp.broadcast_to(jnp.max(peaks[slot], axis=1, keepdims=True) * factor, high.shape)

        def weigh(j):
            _, n, slot = place(j)
            peak = peaks[slot]
            s = s_ref[j]
            e = jnp.concatenate([jnp.exp2(s[:, i * 128:(i + 1) * 128] * factor - peak) for i in range(piece_len // 128)], axis=1)
            v_rows = u[pl.ds(offset(n), piece_len), 2 * head_dim:3 * head_dim]
            return fold(jnp.add, e), jnp.dot(e.astype(jnp.bfloat16), v_rows, preferred_element_type=jnp.float32)

        total, acc = weigh(cp)
        for j in range(cp + 1, pieces + 1):
            more, part = weigh(j)
            total, acc = total + more, acc + part
        totals[0], accs[0] = jnp.zeros_like(total), jnp.zeros_like(acc)
        totals[1], accs[1] = total, acc
        for j in range(cp):
            slot = place(j)[2]
            more, part = weigh(j)
            totals[slot] += more
            accs[slot] += part
        for slot, piece in enumerate((lo, hi)):
            o_st[pl.ds(offset(piece), piece_len), :] = (accs[slot] / jnp.sum(totals[slot], axis=1, keepdims=True)).astype(jnp.bfloat16)
        for i in range(2 * per_half):
            tt = i
            rows = pl.ds(pl.multiple_of(p * 2 * piece_len + i * tokens, tokens), tokens)
            dcl, dtl = (p - c + cp) % cp, (tt - t + tp) % tp
            pl.when(dcl + dtl > 0)(o_copy(rows, dcl, dtl, p, tt).start)

            @pl.when(dcl + dtl == 0)
            def _():
                lanes = pl.ds(pl.multiple_of(unit_head * head_dim, 128), head_dim)
                o_rows[unit_seq, :, lanes] = o_st[rows]

    for dc in (1, cp - 1, 2):
        lane_y[dc].wait_recv()
        lane_mate[dc].start()
    bulk_wave(2)
    bulk_wave(3)
    for i in range(8):
        bulk_sent['p%d' % i].wait_recv()
    for copy in lane_mate.values():
        copy.wait_recv()
    first_rows = pl.ds(0, tokens)
    o_all = [o_copy(first_rows, dc, dt, (c + dc) % cp, (t + dt) % tp) for dc, dt in peers]
    for copy in o_all:
        copy.wait_recv()

    full = tp * heads * head_dim

    @pl.loop(0, hidden // 256)
    def _(n):
        at = pl.ds(pl.multiple_of(n * 256, 256), 256)
        a = jnp.dot(o_rows[...].reshape(2 * tokens, full), wo[:, :, :, at].reshape(full, 256), preferred_element_type=jnp.float32)
        h_ref[:, :, at] = (xg[t, :, :, at].astype(jnp.float32) + a.reshape(2, tokens, 256)).astype(jnp.bfloat16)

    for copy in list(x_sent.values()) + list(bulk_sent.values()) + list(strip_sent.values()) + list(lane_y.values()) + list(lane_mate.values()) + o_all:
        copy.wait_send()
    for dc in (1, cp - 1, 2):
        for tt in range(tp):
            u_copy(dc, tt).wait_send()


def run_front(act_in, w_query, w_key, w_value, w_out, cp, tp, heads):
    n_micro, tokens, hidden = act_in.shape
    head_dim = w_out.shape[1]
    half_rows = tokens * tp
    rows = cp * half_rows
    bf16 = jnp.bfloat16
    any_spec = pl.BlockSpec(memory_space=pl.ANY)
    dma = pltpu.SemaphoreType.DMA
    vmem = [(tp, n_micro, tokens, hidden), (tp // 2, 2, heads * head_dim, hidden), (hidden, heads * 3 * head_dim), (rows, 3 * head_dim), (tp, n_micro, tokens, heads * 3 * head_dim)]
    piece = half_rows // 2
    return pl.pallas_call(
        functools.partial(front_body, cp, tp, heads),
        out_shape=jax.ShapeDtypeStruct(act_in.shape, bf16),
        in_specs=[any_spec] * 5,
        out_specs=pl.BlockSpec(memory_space=pltpu.VMEM),
        scratch_shapes=[pltpu.VMEM(s, bf16) for s in vmem]
        + [pltpu.VMEM((2 * cp + 1, piece, piece), jnp.float32), pltpu.VMEM((rows, head_dim), bf16), pltpu.VMEM((n_micro, tokens, tp * heads * head_dim), bf16)]
        + [pltpu.VMEM((2, piece, 128), jnp.float32), pltpu.VMEM((2, piece, 128), jnp.float32), pltpu.VMEM((2, piece, head_dim), jnp.float32), pltpu.VMEM((3, hidden, heads, head_dim), bf16)]
        + [dma((6,)), dma((2, 14)), dma((2, 14)), dma((2, 14)), dma((2, cp)), dma((2, cp)), dma((2, cp, tp)), dma((2, cp, tp))],
        compiler_params=pltpu.CompilerParams(collective_id=2, has_side_effects=True, vmem_limit_bytes=56 << 20),
        cost_estimate=pl.CostEstimate(flops=8 * rows * hidden * head_dim * 3, bytes_accessed=20 << 20, transcendentals=0),
    )(act_in, w_query, w_key, w_value, w_out.reshape(heads * head_dim, hidden))


def expert_body(cp, tp, cap, h_ref, ids_ref, pick_ref, g_ref, wg_hbm, wu_hbm, wd_hbm, y_ref,
                ids_x, ids_y, g0, g1, s0, s1, e0, e1, z0, z1, b0, b1, f0, f1, wg, wu, wd, rows_in, act, mixed, w_sem,
                idx_sem, idy_sem, ring_x, ring_y, hop_y, hop_x, ret_y, ret_x, fin_x, fin_y):
    d, c, t = lax.axis_index('data'), lax.axis_index('cp'), lax.axis_index('tp')
    tokens, hidden = h_ref.shape[1], h_ref.shape[2]
    ff = wg.shape[1]
    nx = tp // 2
    x, k = t // 2, t % 2
    order = sorted(range(cp), key=lambda i: min(i, cp - i))
    seg = tp * cap
    half = tokens // 2

    weights = [pltpu.make_async_copy(a, b, w_sem.at[i]) for i, (a, b) in enumerate(((wg_hbm, wg), (wu_hbm, wu), (wd_hbm, wd)))]
    for copy in weights:
        copy.start()

    def device(dc, dx, dk):
        return (d, (c + dc) % cp, ((x + dx) % nx) * 2 + (k + dk) % 2)

    row_peers = [(dx, dk) for dx in order for dk in (0, 1) if dx or dk]
    col_peers = [(dc, dk) for dc in order for dk in (0, 1) if dc or dk]
    barrier = pltpu.get_barrier_semaphore()
    peers = [(0, dx, dk) for dx, dk in row_peers] + [(dc, 0, dk) for dc, dk in col_peers if dc]
    for peer in peers:
        pl.semaphore_signal(barrier, inc=1, device_id=device(*peer), device_id_type=MESH_ID)
    pl.semaphore_wait(barrier, len(peers))

    def send(src, dst, sems, key, target):
        return pltpu.make_async_remote_copy(src_ref=src, dst_ref=dst, send_sem=sems.at[(0,) + key], recv_sem=sems.at[(1,) + key], device_id=target, device_id_type=MESH_ID)

    started = []

    def go(*args):
        copy = send(*args)
        copy.start()
        started.append(copy)
        return copy

    ids_sent = {}
    for i in order[1:]:
        ids_sent[0, i] = go(ids_ref, ids_x.at[x], idx_sem, (i,), device(0, i, 0))
        ids_sent[1, i] = go(ids_ref, ids_y.at[c], idy_sem, (i,), device(i, 0, 0))

    parts = (pl.ds(0, half), pl.ds(half, half))
    ahead = (device(0, 1, 0), device(1, 0, 0))
    behind = (device(0, nx - 1, 0), device(cp - 1, 0, 0))
    here, size = (x, c), (nx, cp)
    held, sems = (g0, g1), (ring_x, ring_y)
    ring = {}
    for b in range(2):
        ring[b, 'r0'] = go(h_ref.at[b, parts[0]], held[b].at[here[b], parts[0]], sems[b], (0,), ahead[b])
        ring[b, 'l0'] = go(h_ref.at[b, parts[1]], held[b].at[here[b], parts[1]], sems[b], (1,), behind[b])
        ring[b, 'r1'] = go(h_ref.at[b, parts[1]], held[b].at[here[b], parts[1]], sems[b], (2,), ahead[b])
        ring[b, 'l1'] = go(h_ref.at[b, parts[0]], held[b].at[here[b], parts[0]], sems[b], (3,), behind[b])

    def relay(b):
        prev, nxt = (here[b] + size[b] - 1) % size[b], (here[b] + 1) % size[b]
        ring[b, 'r0'].wait_recv()
        ring[b, 'r2'] = go(held[b].at[prev, parts[0]], held[b].at[prev, parts[0]], sems[b], (4,), ahead[b])
        ring[b, 'l0'].wait_recv()
        ring[b, 'l2'] = go(held[b].at[nxt, parts[1]], held[b].at[nxt, parts[1]], sems[b], (5,), behind[b])

    slot_row = lax.broadcasted_iota(jnp.int32, (seg, tokens), 0)
    group = 2 * cap
    wanted = ((slot_row // group * (tp * cap) + x * group + slot_row % group).astype(jnp.float32), (slot_row + c * seg).astype(jnp.float32))
    hop = {}

    def stage(b, step):
        back = order[step]
        src = (here[b] + size[b] - back) % size[b]
        out = (s0, s1)[b]
        if step:
            ids_sent[b, back].wait_recv()
            ids = (ids_x, ids_y)[b][src]
        else:
            ids = ids_ref[...]
        hit = (ids[2 * b:2 * b + 1] == wanted[b]) | (ids[2 * b + 1:2 * b + 2] == wanted[b])
        sel = jnp.where(hit, 1.0, 0.0).astype(jnp.bfloat16)

        @pl.loop(0, hidden // 512)
        def _(n):
            at = pl.ds(pl.multiple_of(n * 512, 512), 512)
            rows = held[b][src, :, at] if step else h_ref[b, :, at]
            got = jnp.dot(sel, rows, preferred_element_type=jnp.float32).astype(jnp.bfloat16)
            out[step, :, :, :, at] = got.reshape(out.shape[1:4] + (512,))

        if b == 0:
            for dc, dk in col_peers:
                target = device(dc, 0, dk)
                hop[0, step, dc, dk] = go(s0.at[step, target[1], (k + dk) % 2], e0.at[src, c, k], hop_y, (step, dc, dk), target)
            e0[src, c, k] = s0[step, c, k]
        else:
            for dx, dk in row_peers:
                target = device(0, dx, dk)
                hop[1, step, dx, dk] = go(s1.at[step, (x + dx) % nx, (k + dk) % 2], e1.at[src, x, k], hop_x, (step, dx, dk), target)
            e1[src, x, k] = s1[step, x, k]

    stage(0, 0)
    stage(1, 0)
    relay(0)
    relay(1)
    for b in range(2):
        ring[b, 'r1'].wait_recv()
        stage(b, 1)
    for b in range(2):
        ring[b, 'l1'].wait_recv()
        stage(b, 2)
    for b in range(2):
        ring[b, 'r2'].wait_recv()
        ring[b, 'l2'].wait_recv()
        stage(b, 3)
    for copy in weights:
        copy.wait()

    def hidden_tile(at, width):
        both = jnp.dot(rows_in[...], jnp.concatenate([wg[:, at], wu[:, at]], axis=1), preferred_element_type=jnp.float32)
        gate, up = both[:, :width], both[:, width:]
        act[:, at] = (jax.nn.silu(gate) * up).astype(jnp.bfloat16)

    def run_expert():
        @pl.loop(0, ff // 256)
        def _(n):
            hidden_tile(pl.ds(pl.multiple_of(n * 256, 256), 256), 256)

        if ff % 256:
            hidden_tile(pl.ds(ff // 256 * 256, ff % 256), ff % 256)

        @pl.loop(0, hidden // 512)
        def _(n):
            at = pl.ds(pl.multiple_of(n * 512, 512), 512)
            rows_in[:, at] = jnp.dot(act[...], wd[:, at], preferred_element_type=jnp.float32).astype(jnp.bfloat16)

    ret = {}
    for step in range(cp):
        xs, cs = (x + nx - order[step]) % nx, (c + cp - order[step]) % cp
        for dc, dk in col_peers:
            hop[0, step, dc, dk].wait_recv()
        for dx, dk in row_peers:
            hop[1, step, dx, dk].wait_recv()
        rows_in[0:seg] = e0[xs].reshape(seg, hidden)
        rows_in[seg:2 * seg] = e1[cs].reshape(seg, hidden)
        run_expert()
        z0[step] = rows_in[0:seg].reshape(cp, 2, cap, hidden)
        z1[step] = rows_in[seg:2 * seg].reshape(nx, 2, cap, hidden)
        for dc, dk in col_peers:
            target = device(dc, 0, dk)
            ret[0, step, dc, dk] = go(z0.at[step, target[1], (k + dk) % 2], b0.at[step, c, k], ret_y, (step, dc, dk), target)
        b0[step, c, k] = z0[step, c, k]
        for dx, dk in row_peers:
            target = device(0, dx, dk)
            ret[1, step, dx, dk] = go(z1.at[step, (x + dx) % nx, (k + dk) % 2], b1.at[step, x, k], ret_x, (step, dx, dk), target)
        b1[step, x, k] = z1[step, x, k]

    fin = {}
    for step in range(cp):
        back = order[step]
        for dc, dk in col_peers:
            ret[0, step, dc, dk].wait_recv()
        if step:
            fin[0, step] = go(b0.at[step], f0.at[x], fin_x, (step,), device(0, nx - back, 0))
        for dx, dk in row_peers:
            ret[1, step, dx, dk].wait_recv()
        if step:
            fin[1, step] = go(b1.at[step], f1.at[c], fin_y, (step,), device(cp - back, 0, 0))

    for step in range(cp):
        if step:
            fin[0, step].wait_recv()
            fin[1, step].wait_recv()

        @pl.loop(0, hidden // 512)
        def _(n):
            at = pl.ds(pl.multiple_of(n * 512, 512), 512)
            for b in range(2):
                src = (here[b] + order[step]) % size[b]
                rows = (f0, f1)[b][src, :, :, :, at] if step else (b0, b1)[b][0, :, :, :, at]
                pick = pick_ref[b, :, pl.ds(pl.multiple_of(src * seg, seg), seg)]
                got = jnp.dot(pick, rows.reshape(seg, 512), preferred_element_type=jnp.float32)
                if step:
                    got += mixed[b, :, at]
                if step < cp - 1:
                    mixed[b, :, at] = got
                else:
                    both = g_ref[b, :, 0:1] * got[:tokens] + g_ref[b, :, 1:2] * got[tokens:]
                    y_ref[b, :, at] = (h_ref[b, :, at].astype(jnp.float32) + both).astype(jnp.bfloat16)

    for copy in started:
        copy.wait_send()


def run_experts(mid_rows, ids, pick, route_gates, w_gate, w_up, w_down, cp, tp, cap):
    n_micro, tokens, hidden = mid_rows.shape
    ff = w_gate.shape[1]
    bf16 = jnp.bfloat16
    nx = tp // 2
    by_x, by_y = (cp, cp, 2, cap, hidden), (cp, nx, 2, cap, hidden)
    rows = 2 * (tp * cap)
    vmem = pl.BlockSpec(memory_space=pltpu.VMEM)
    any_spec = pl.BlockSpec(memory_space=pl.ANY)
    dma = pltpu.SemaphoreType.DMA
    return pl.pallas_call(
        functools.partial(expert_body, cp, tp, cap),
        out_shape=jax.ShapeDtypeStruct(mid_rows.shape, bf16),
        in_specs=[vmem] * 4 + [any_spec] * 3,
        out_specs=vmem,
        scratch_shapes=[pltpu.VMEM((nx,) + ids.shape, jnp.float32), pltpu.VMEM((cp,) + ids.shape, jnp.float32)]
        + [pltpu.VMEM((nx, tokens, hidden), bf16), pltpu.VMEM((cp, tokens, hidden), bf16)]
        + [pltpu.VMEM(s, bf16) for s in (by_x, by_y) * 5]
        + [pltpu.VMEM((hidden, ff), bf16), pltpu.VMEM((hidden, ff), bf16), pltpu.VMEM((ff, hidden), bf16)]
        + [pltpu.VMEM((rows, hidden), bf16), pltpu.VMEM((rows, ff), bf16), pltpu.VMEM((n_micro, 2 * tokens, hidden), jnp.float32)]
        + [dma((3,)), dma((2, nx)), dma((2, cp)), dma((2, 6)), dma((2, 6)), dma((2, cp, cp, 2)), dma((2, cp, nx, 2)), dma((2, cp, cp, 2)), dma((2, cp, nx, 2)), dma((2, cp)), dma((2, cp))],
        compiler_params=pltpu.CompilerParams(collective_id=1, has_side_effects=True, vmem_limit_bytes=60 << 20),
        cost_estimate=pl.CostEstimate(flops=6 * 4 * rows * hidden * ff, bytes_accessed=6 * hidden * ff, transcendentals=0),
    )(mid_rows, ids, pick, route_gates, w_gate, w_up, w_down)


def solution(mesh):
    cp_size = mesh.shape['cp']
    tp_size = mesh.shape['tp']
    experts = cp_size * tp_size
    row_spec = P(None, ('data', 'cp', 'tp'), None)
    head_spec = P(None, 'tp', None)
    out_spec = P('tp', None, None)
    expert_spec = P(('cp', 'tp'), None, None)

    def device_step(act_in, route_ids, route_gates, w_query, w_key, w_value, w_out, w_gate, w_up, w_down):
        n_micro, tokens, hidden = act_in.shape
        heads, head_dim = w_query.shape[1], w_query.shape[2]
        mid_rows = run_front(act_in, w_query, w_key, w_value, w_out, cp_size, tp_size, heads)

        capacity = (4 * tokens) // experts
        slots = experts * capacity
        flat_ids = route_ids.reshape(n_micro, 2 * tokens)
        hits = (flat_ids[..., None] == jnp.arange(experts)).astype(jnp.bfloat16)
        before = (jnp.arange(2 * tokens)[:, None] > jnp.arange(2 * tokens)[None, :]).astype(jnp.bfloat16)
        rank = jnp.einsum('ij,bje->bie', before, hits, preferred_element_type=jnp.float32)
        slot_rank = jnp.sum(rank * hits.astype(jnp.float32), axis=-1).astype(jnp.int32)
        col, row = flat_ids % tp_size, flat_ids // tp_size
        chip_slot = ((col // 2 * cp_size + row) * 2 + col % 2) * capacity
        base_slot = jnp.where(jnp.arange(n_micro)[:, None] == 0, chip_slot, flat_ids * capacity)
        by_choice = lambda v: v.reshape(n_micro, tokens, 2).transpose(0, 2, 1).reshape(n_micro, 2 * tokens)
        pick = (by_choice(base_slot + slot_rank)[:, :, None] == jnp.arange(slots)).astype(jnp.bfloat16)
        ids = by_choice(flat_ids * capacity + slot_rank).astype(jnp.float32).reshape(2 * n_micro, tokens)
        ids = jnp.concatenate([ids, ids], axis=0)
        return run_experts(mid_rows, ids, pick, route_gates, w_gate[0], w_up[0], w_down[0], cp_size, tp_size, capacity)

    return jax.shard_map(device_step, mesh=mesh, in_specs=(row_spec, row_spec, row_spec, head_spec, head_spec, head_spec, out_spec, expert_spec, expert_spec, expert_spec), out_specs=row_spec, check_vma=False)
```

```python
import functools

import jax
import jax.numpy as jnp
from jax import lax
from jax.experimental import pallas as pl
from jax.experimental.pallas import tpu as pltpu
from jax.sharding import PartitionSpec as P

LOG2E = 1.4426950408889634


MESH_ID = pl.DeviceIdType.MESH


def front_body(cp, tp, heads, strip_len, x_hbm, wq_hbm, wk_hbm, wv_hbm, wo_hbm, h_ref, xg, wo, w, u, q_out, s_ref, o_st, o_rows,
               peaks, totals, accs, raw, a_sum, in_sem, x_sem, bulk_sem, strip_sem, lane_sem, mate_sem, u_sem, o_sem):
    d, c, t = lax.axis_index('data'), lax.axis_index('cp'), lax.axis_index('tp')
    nx = tp // 2
    x, k = t // 2, t % 2
    tokens, hidden = x_hbm.shape[1], x_hbm.shape[2]
    half_rows = tokens * tp
    pieces = 2 * cp
    piece_len = half_rows // 2
    head_dim = o_st.shape[1]
    width = 3 * head_dim
    left, right, far = ((x + nx - 1) % nx) * 2, ((x + 1) % nx) * 2, ((x + 2) % nx) * 2
    mine, other = k, 1 - k
    mate = 2 * x + other

    split = wo_hbm.shape[0] - strip_len * cp
    strip_rows = pl.ds(split + strip_len * c, strip_len)
    loads = [pltpu.make_async_copy(x_hbm, xg.at[t], in_sem.at[0]), pltpu.make_async_copy(wq_hbm, raw.at[0], in_sem.at[1]), pltpu.make_async_copy(wo_hbm.at[pl.ds(0, split)], wo.at[x, k, pl.ds(0, split)], in_sem.at[2]),
             pltpu.make_async_copy(wo_hbm.at[strip_rows], wo.at[x, k, strip_rows], in_sem.at[3]),
             pltpu.make_async_copy(wk_hbm, raw.at[1], in_sem.at[4]), pltpu.make_async_copy(wv_hbm, raw.at[2], in_sem.at[5])]
    for load in loads:
        load.start()
    barrier = pltpu.get_barrier_semaphore()
    peers = [(dc, dt) for dc in range(cp) for dt in range(tp) if dc or dt]
    for dc, dt in peers:
        pl.semaphore_signal(barrier, inc=1, device_id=(d, (c + dc) % cp, (t + dt) % tp), device_id_type=MESH_ID)
    pl.semaphore_wait(barrier, len(peers))

    def send(src, dst, sems, key, cc, tt):
        return pltpu.make_async_remote_copy(src_ref=src, dst_ref=dst, send_sem=sems.at[(0,) + key], recv_sem=sems.at[(1,) + key], device_id=(d, cc, tt), device_id_type=MESH_ID)

    names = ['r0', 'r1', 'r2', 'l0', 'l1', 'l2'] + ['p%d' % i for i in range(8)]

    def ring(view, sems, with_mate):
        sent = {}

        def start(name, src, part, target):
            if with_mate or name[0] != 'p':
                sent[name] = send(view(src, part), view(src, part), sems, (names.index(name),), c, target)
                sent[name].start()

        def wave(n):
            if n == 0:
                start('p0', t, 0, mate)
                start('p1', t, 1, mate)
                start('r0', t, 0, right + mine)
                start('l0', t, 1, left + mine)
                start('r1', t, 1, right + mine)
                start('l1', t, 0, left + mine)
            elif n == 1:
                sent['r0'].wait_recv()
                start('r2', left + mine, 0, right + mine)
                start('p2', left + mine, 0, mate)
                sent['l0'].wait_recv()
                start('l2', right + mine, 1, left + mine)
                start('p3', right + mine, 1, mate)
            elif n == 2:
                sent['r1'].wait_recv()
                start('p4', left + mine, 1, mate)
                sent['l1'].wait_recv()
                start('p5', right + mine, 0, mate)
            else:
                sent['r2'].wait_recv()
                start('p6', far + mine, 0, mate)
                sent['l2'].wait_recv()
                start('p7', far + mine, 1, mate)
        return sent, wave

    part_rows = split // 2

    def bulk(src, part):
        return wo.at[src // 2, src % 2, pl.ds(part * part_rows, part_rows)]

    def strip(src, part):
        return wo.at[src // 2, src % 2, pl.ds(split + strip_len * c, strip_len), pl.ds(part * (hidden // 2), hidden // 2)]

    def lane(q):
        return wo.at[:, k, pl.ds(split + strip_len * q, strip_len)]

    x_sent, x_wave = ring(lambda src, part: xg.at[src, part], x_sem, True)
    bulk_sent, bulk_wave = ring(bulk, bulk_sem, True)
    strip_sent, strip_wave = ring(strip, strip_sem, False)
    lane_y = {dc: send(lane(c), lane(c), lane_sem, (dc,), (c + dc) % cp, t) for dc in (1, cp - 1, 2)}
    lane_mate = {dc: send(lane((c + cp - dc) % cp), lane((c + cp - dc) % cp), mate_sem, (dc,), c, mate) for dc in (0, 1, cp - 1, 2)}

    def project(tt, s):
        @pl.loop(0, heads * width // 256)
        def _(n):
            at = pl.ds(pl.multiple_of(n * 256, 256), 256)
            q_out[tt, s, :, at] = jnp.dot(xg[tt, s], w[:, at], preferred_element_type=jnp.float32).astype(jnp.bfloat16)

        rows = pl.ds(pl.multiple_of(c * half_rows + tt * tokens, tokens), tokens)
        for dc in (1, cp - 1, 2):
            c2 = (c + dc) % cp
            lanes = pl.ds(pl.multiple_of(c2 % heads * width, 128), width)
            copy = send(q_out.at[tt, s, :, lanes], u.at[rows], u_sem, (dc, tt), c2, t)
            pl.when(c2 // heads == s)(copy.start)

        @pl.when(c // heads == s)
        def _():
            lanes = pl.ds(pl.multiple_of(c % heads * width, 128), width)
            u[rows] = q_out[tt, s, :, lanes]

    def relayout(j, load):
        load.wait()

        @pl.loop(0, hidden // 32)
        def _(i):
            at = pl.ds(pl.multiple_of(i * 32, 32), 32)
            flat = raw[j, at].reshape(32, heads * head_dim)
            for n in range(heads):
                w[at, n * width + j * head_dim:n * width + (j + 1) * head_dim] = flat[:, n * head_dim:(n + 1) * head_dim]

    loads[3].wait()
    strip_wave(0)
    relayout(0, loads[1])
    strip_wave(1)
    loads[0].wait()
    x_wave(0)
    relayout(1, loads[4])
    relayout(2, loads[5])
    project(t, 0)
    project(t, 1)
    for s, name in ((0, 'p0'), (1, 'p1')):
        x_sent[name].wait_recv()
        project(mate, s)
    x_wave(1)
    project(left + mine, 0)
    project(right + mine, 1)
    x_sent['p2'].wait_recv()
    project(left + other, 0)
    x_sent['p3'].wait_recv()
    project(right + other, 1)
    x_wave(2)
    loads[2].wait()
    bulk_wave(0)
    project(left + mine, 1)
    project(right + mine, 0)
    x_sent['p4'].wait_recv()
    project(left + other, 1)
    x_sent['p5'].wait_recv()
    project(right + other, 0)
    x_wave(3)
    project(far + mine, 0)
    project(far + mine, 1)
    x_sent['p6'].wait_recv()
    project(far + other, 0)
    x_sent['p7'].wait_recv()
    project(far + other, 1)
    strip_wave(2)
    strip_wave(3)
    for dc in (1, cp - 1, 2):
        lane_y[dc].start()
    lane_mate[0].start()

    def u_copy(dc, tt):
        c2 = (c + dc) % cp
        lanes = pl.ds(pl.multiple_of(c2 % heads * width, 128), width)
        rows = pl.ds(pl.multiple_of(c * half_rows + tt * tokens, tokens), tokens)
        return send(q_out.at[tt, c2 // heads, :, lanes], u.at[rows], u_sem, (dc, tt), c2, t)

    for dc in (1, cp - 1, 2):
        for tt in range(tp):
            u_copy(dc, tt).wait_recv()
    bulk_wave(1)

    factor = head_dim ** -0.5 * LOG2E
    per_half = tp // 2

    def offset(n):
        return pl.multiple_of(jnp.where(n < cp, 2 * piece_len * n, 2 * piece_len * (pieces - 1 - n) + piece_len), piece_len)

    def fold(op, wide):
        parts = [wide[:, i * 128:(i + 1) * 128] for i in range(piece_len // 128)]
        while len(parts) > 1:
            parts = [op(a, b) for a, b in zip(parts[::2], parts[1::2])]
        return parts[0]

    row = lax.broadcasted_iota(jnp.int32, (piece_len, piece_len), 0)
    col = lax.broadcasted_iota(jnp.int32, (piece_len, piece_len), 1)
    unit_seq = c // heads
    unit_head = t * heads + c % heads

    def o_copy(rows, dcl, dtl, cc, tt):
        lanes = pl.ds(pl.multiple_of(unit_head * head_dim, 128), head_dim)
        return send(o_st.at[rows], o_rows.at[unit_seq, :, lanes], o_sem, (dcl, dtl), cc, tt)

    gap = col - row

    @pl.loop(0, cp)
    def _(p):
        lo, hi = p, pieces - 1 - p

        def place(j):
            if j >= cp:
                return hi, j - p - 1, 1
            is_lo = j <= p
            return jnp.where(is_lo, lo, hi), jnp.where(is_lo, j, j - p - 1), jnp.where(is_lo, 0, 1)

        def scores(j):
            piece, n, _ = place(j)
            q_rows = u[pl.ds(offset(piece), piece_len), 0:head_dim]
            k_rows = u[pl.ds(offset(n), piece_len), head_dim:2 * head_dim]
            s = lax.dot_general(q_rows, k_rows, (((1,), (1,)), ((), ())), preferred_element_type=jnp.float32)
            if j == pieces:
                s = jnp.where(gap <= 0, s, -jnp.inf)
            elif j < cp:
                s = jnp.where(gap <= jnp.where(j == p, 0, piece_len), s, -jnp.inf)
            s_ref[j] = s
            return fold(jnp.maximum, s)

        high = scores(cp)
        for j in range(cp + 1, pieces + 1):
            high = jnp.maximum(high, scores(j))
        peaks[1] = high
        peaks[0] = jnp.full_like(high, -jnp.inf)
        for j in range(cp):
            slot = place(j)[2]
            peaks[slot] = jnp.maximum(peaks[slot], scores(j))
        for slot in range(2):
            peaks[slot] = jnp.broadcast_to(jnp.max(peaks[slot], axis=1, keepdims=True) * factor, high.shape)

        def weigh(j):
            _, n, slot = place(j)
            peak = peaks[slot]
            s = s_ref[j]
            e = jnp.concatenate([jnp.exp2(s[:, i * 128:(i + 1) * 128] * factor - peak) for i in range(piece_len // 128)], axis=1)
            v_rows = u[pl.ds(offset(n), piece_len), 2 * head_dim:3 * head_dim]
            return fold(jnp.add, e), jnp.dot(e.astype(jnp.bfloat16), v_rows, preferred_element_type=jnp.float32)

        total, acc = weigh(cp)
        for j in range(cp + 1, pieces + 1):
            more, part = weigh(j)
            total, acc = total + more, acc + part
        totals[0], accs[0] = jnp.zeros_like(total), jnp.zeros_like(acc)
        totals[1], accs[1] = total, acc
        for j in range(cp):
            slot = place(j)[2]
            more, part = weigh(j)
            totals[slot] += more
            accs[slot] += part
        for slot, piece in enumerate((lo, hi)):
            o_st[pl.ds(offset(piece), piece_len), :] = (accs[slot] / jnp.sum(totals[slot], axis=1, keepdims=True)).astype(jnp.bfloat16)
        for i in range(2 * per_half):
            tt = i
            rows = pl.ds(pl.multiple_of(p * 2 * piece_len + i * tokens, tokens), tokens)
            dcl, dtl = (p - c + cp) % cp, (tt - t + tp) % tp
            pl.when(dcl + dtl > 0)(o_copy(rows, dcl, dtl, p, tt).start)

            @pl.when(dcl + dtl == 0)
            def _():
                lanes = pl.ds(pl.multiple_of(unit_head * head_dim, 128), head_dim)
                o_rows[unit_seq, :, lanes] = o_st[rows]

    for dc in (1, cp - 1, 2):
        lane_y[dc].wait_recv()
        lane_mate[dc].start()
    bulk_wave(2)
    first_rows = pl.ds(0, tokens)
    o_all = [o_copy(first_rows, dc, dt, (c + dc) % cp, (t + dt) % tp) for dc, dt in peers]
    per_chip = 2 * heads * head_dim

    def contract(dx, names):
        xs = (x + nx - dx) % nx
        for name in names:
            bulk_sent[name].wait_recv()
        for dc in range(cp):
            for dk in range(2):
                if dx or dc or dk:
                    dt = (t + tp - 2 * xs - (k + dk) % 2) % tp
                    o_copy(first_rows, dc, dt, (c + dc) % cp, (t + dt) % tp).wait_recv()

        @pl.loop(0, hidden // 512)
        def _(n):
            at = pl.ds(pl.multiple_of(n * 512, 512), 512)
            o_part = o_rows[:, :, pl.ds(pl.multiple_of(xs * per_chip, per_chip), per_chip)].reshape(2 * tokens, per_chip)
            a = jnp.dot(o_part, wo[xs, :, :, at].reshape(per_chip, 512), preferred_element_type=jnp.float32)
            if dx:
                a += a_sum[:, at]
            if dx == 2:
                h_ref[:, :, at] = (xg[t, :, :, at].astype(jnp.float32) + a.reshape(2, tokens, 512)).astype(jnp.bfloat16)
            else:
                a_sum[:, at] = a

    for copy in lane_mate.values():
        copy.wait_recv()
    contract(0, ('p0', 'p1'))
    bulk_wave(3)
    contract(1, ('p2', 'p4'))
    contract(nx - 1, ('p3', 'p5'))
    contract(2, ('p6', 'p7'))

    for copy in list(x_sent.values()) + list(bulk_sent.values()) + list(strip_sent.values()) + list(lane_y.values()) + list(lane_mate.values()) + o_all:
        copy.wait_send()
    for dc in (1, cp - 1, 2):
        for tt in range(tp):
            u_copy(dc, tt).wait_send()


def run_front(act_in, w_query, w_key, w_value, w_out, cp, tp, heads):
    n_micro, tokens, hidden = act_in.shape
    head_dim = w_out.shape[1]
    half_rows = tokens * tp
    rows = cp * half_rows
    bf16 = jnp.bfloat16
    any_spec = pl.BlockSpec(memory_space=pl.ANY)
    dma = pltpu.SemaphoreType.DMA
    vmem = [(tp, n_micro, tokens, hidden), (tp // 2, 2, heads * head_dim, hidden), (hidden, heads * 3 * head_dim), (rows, 3 * head_dim), (tp, n_micro, tokens, heads * 3 * head_dim)]
    piece = half_rows // 2
    return pl.pallas_call(
        functools.partial(front_body, cp, tp, heads, 16),
        out_shape=jax.ShapeDtypeStruct(act_in.shape, bf16),
        in_specs=[any_spec] * 5,
        out_specs=pl.BlockSpec(memory_space=pltpu.VMEM),
        scratch_shapes=[pltpu.VMEM(s, bf16) for s in vmem]
        + [pltpu.VMEM((2 * cp + 1, piece, piece), jnp.float32), pltpu.VMEM((rows, head_dim), bf16), pltpu.VMEM((n_micro, tokens, tp * heads * head_dim), bf16)]
        + [pltpu.VMEM((2, piece, 128), jnp.float32), pltpu.VMEM((2, piece, 128), jnp.float32), pltpu.VMEM((2, piece, head_dim), jnp.float32), pltpu.VMEM((3, hidden, heads, head_dim), bf16), pltpu.VMEM((n_micro * tokens, hidden), jnp.float32)]
        + [dma((6,)), dma((2, 14)), dma((2, 14)), dma((2, 14)), dma((2, cp)), dma((2, cp)), dma((2, cp, tp)), dma((2, cp, tp))],
        compiler_params=pltpu.CompilerParams(collective_id=2, has_side_effects=True, vmem_limit_bytes=56 << 20),
        cost_estimate=pl.CostEstimate(flops=8 * rows * hidden * head_dim * 3, bytes_accessed=20 << 20, transcendentals=0),
    )(act_in, w_query, w_key, w_value, w_out.reshape(heads * head_dim, hidden))


def expert_body(cp, tp, cap, h_ref, route_ref, g_ref, wg_hbm, wu_hbm, wd_hbm, y_ref,
                ids_ref, pos_ref, ids_x, ids_y, g0, g1, s0, s1, e0, e1, z0, z1, b0, b1, f0, f1, wg, wu, wd, rows_in, act, mixed, w_sem,
                idx_sem, idy_sem, ring_x, ring_y, hop_y, hop_x, ret_y, ret_x, fin_x, fin_y):
    d, c, t = lax.axis_index('data'), lax.axis_index('cp'), lax.axis_index('tp')
    tokens, hidden = h_ref.shape[1], h_ref.shape[2]
    ff = wg.shape[1]
    nx = tp // 2
    x, k = t // 2, t % 2
    order = sorted(range(cp), key=lambda i: min(i, cp - i))
    seg = tp * cap
    half = tokens // 2

    weights = [pltpu.make_async_copy(a, b, w_sem.at[i]) for i, (a, b) in enumerate(((wg_hbm, wg), (wu_hbm, wu), (wd_hbm, wd)))]
    for copy in weights:
        copy.start()

    def device(dc, dx, dk):
        return (d, (c + dc) % cp, ((x + dx) % nx) * 2 + (k + dk) % 2)

    row_peers = [(dx, dk) for dx in order for dk in (0, 1) if dx or dk]
    col_peers = [(dc, dk) for dc in order for dk in (0, 1) if dc or dk]
    barrier = pltpu.get_barrier_semaphore()
    peers = [(0, dx, dk) for dx, dk in row_peers] + [(dc, 0, dk) for dc, dk in col_peers if dc]
    for peer in peers:
        pl.semaphore_signal(barrier, inc=1, device_id=device(*peer), device_id_type=MESH_ID)
    experts = cp * tp
    expert = lax.broadcasted_iota(jnp.int32, (experts, tokens), 0)
    before = lax.broadcasted_iota(jnp.int32, (tokens, tokens), 0) < lax.broadcasted_iota(jnp.int32, (tokens, tokens), 1)
    before = jnp.where(before, 1.0, 0.0).astype(jnp.bfloat16)
    e_col, e_row = expert % tp, expert // tp
    bases = ((((e_col // 2 * cp + e_row) * 2 + e_col % 2) * cap).astype(jnp.float32), (expert * cap).astype(jnp.float32))
    ids_ref[...] = jnp.zeros_like(ids_ref)
    for b in range(2):
        used = jnp.zeros((experts, 1), jnp.float32)
        for i in range(2):
            row = 2 * b + i
            hit = jnp.where(expert == route_ref[b, i:i + 1, :], 1.0, 0.0)
            rank = jnp.dot(hit.astype(jnp.bfloat16), before, preferred_element_type=jnp.float32) + used
            used = used + jnp.sum(hit, axis=1, keepdims=True)
            ids_ref[row:row + 1] = jnp.sum(hit * (rank + bases[1]), axis=0, keepdims=True)
            pos_ref[row:row + 1] = jnp.sum(hit * (rank + bases[b]), axis=0, keepdims=True)
    pl.semaphore_wait(barrier, len(peers))

    def send(src, dst, sems, key, target):
        return pltpu.make_async_remote_copy(src_ref=src, dst_ref=dst, send_sem=sems.at[(0,) + key], recv_sem=sems.at[(1,) + key], device_id=target, device_id_type=MESH_ID)

    started = []

    def go(*args):
        copy = send(*args)
        copy.start()
        started.append(copy)
        return copy

    ids_sent = {}
    for i in order[1:]:
        ids_sent[0, i] = go(ids_ref, ids_x.at[x], idx_sem, (i,), device(0, i, 0))
        ids_sent[1, i] = go(ids_ref, ids_y.at[c], idy_sem, (i,), device(i, 0, 0))

    parts = (pl.ds(0, half), pl.ds(half, half))
    ahead = (device(0, 1, 0), device(1, 0, 0))
    behind = (device(0, nx - 1, 0), device(cp - 1, 0, 0))
    here, size = (x, c), (nx, cp)
    held, sems = (g0, g1), (ring_x, ring_y)
    ring = {}
    for b in range(2):
        ring[b, 'r0'] = go(h_ref.at[b, parts[0]], held[b].at[here[b], parts[0]], sems[b], (0,), ahead[b])
        ring[b, 'l0'] = go(h_ref.at[b, parts[1]], held[b].at[here[b], parts[1]], sems[b], (1,), behind[b])
        ring[b, 'r1'] = go(h_ref.at[b, parts[1]], held[b].at[here[b], parts[1]], sems[b], (2,), ahead[b])
        ring[b, 'l1'] = go(h_ref.at[b, parts[0]], held[b].at[here[b], parts[0]], sems[b], (3,), behind[b])

    def relay(b):
        prev, nxt = (here[b] + size[b] - 1) % size[b], (here[b] + 1) % size[b]
        ring[b, 'r0'].wait_recv()
        ring[b, 'r2'] = go(held[b].at[prev, parts[0]], held[b].at[prev, parts[0]], sems[b], (4,), ahead[b])
        ring[b, 'l0'].wait_recv()
        ring[b, 'l2'] = go(held[b].at[nxt, parts[1]], held[b].at[nxt, parts[1]], sems[b], (5,), behind[b])

    slot_row = lax.broadcasted_iota(jnp.int32, (seg, tokens), 0)
    group = 2 * cap
    wanted = ((slot_row // group * (tp * cap) + x * group + slot_row % group).astype(jnp.float32), (slot_row + c * seg).astype(jnp.float32))
    hop = {}

    def stage(b, step):
        back = order[step]
        src = (here[b] + size[b] - back) % size[b]
        out = (s0, s1)[b]
        if step:
            ids_sent[b, back].wait_recv()
            ids = (ids_x, ids_y)[b][src]
        else:
            ids = ids_ref[...]
        hit = (ids[2 * b:2 * b + 1] == wanted[b]) | (ids[2 * b + 1:2 * b + 2] == wanted[b])
        sel = jnp.where(hit, 1.0, 0.0).astype(jnp.bfloat16)

        @pl.loop(0, hidden // 512)
        def _(n):
            at = pl.ds(pl.multiple_of(n * 512, 512), 512)
            rows = held[b][src, :, at] if step else h_ref[b, :, at]
            got = jnp.dot(sel, rows, preferred_element_type=jnp.float32).astype(jnp.bfloat16)
            out[step, :, :, :, at] = got.reshape(out.shape[1:4] + (512,))

        if b == 0:
            for dc, dk in col_peers:
                target = device(dc, 0, dk)
                hop[0, step, dc, dk] = go(s0.at[step, target[1], (k + dk) % 2], e0.at[src, c, k], hop_y, (step, dc, dk), target)
            e0[src, c, k] = s0[step, c, k]
        else:
            for dx, dk in row_peers:
                target = device(0, dx, dk)
                hop[1, step, dx, dk] = go(s1.at[step, (x + dx) % nx, (k + dk) % 2], e1.at[src, x, k], hop_x, (step, dx, dk), target)
            e1[src, x, k] = s1[step, x, k]

    stage(0, 0)
    stage(1, 0)
    relay(0)
    relay(1)
    for b in range(2):
        ring[b, 'r1'].wait_recv()
        stage(b, 1)
    for b in range(2):
        ring[b, 'l1'].wait_recv()
        stage(b, 2)
    for b in range(2):
        ring[b, 'r2'].wait_recv()
        ring[b, 'l2'].wait_recv()
        stage(b, 3)
    for copy in weights:
        copy.wait()

    def hidden_tile(at, width):
        both = jnp.dot(rows_in[...], jnp.concatenate([wg[:, at], wu[:, at]], axis=1), preferred_element_type=jnp.float32)
        gate, up = both[:, :width], both[:, width:]
        act[:, at] = (jax.nn.silu(gate) * up).astype(jnp.bfloat16)

    def run_expert():
        @pl.loop(0, ff // 256)
        def _(n):
            hidden_tile(pl.ds(pl.multiple_of(n * 256, 256), 256), 256)

        if ff % 256:
            hidden_tile(pl.ds(ff // 256 * 256, ff % 256), ff % 256)

        @pl.loop(0, hidden // 512)
        def _(n):
            at = pl.ds(pl.multiple_of(n * 512, 512), 512)
            rows_in[:, at] = jnp.dot(act[...], wd[:, at], preferred_element_type=jnp.float32).astype(jnp.bfloat16)

    ret = {}
    for step in range(cp):
        xs, cs = (x + nx - order[step]) % nx, (c + cp - order[step]) % cp
        for dc, dk in col_peers:
            hop[0, step, dc, dk].wait_recv()
        for dx, dk in row_peers:
            hop[1, step, dx, dk].wait_recv()
        rows_in[0:seg] = e0[xs].reshape(seg, hidden)
        rows_in[seg:2 * seg] = e1[cs].reshape(seg, hidden)
        run_expert()
        z0[step] = rows_in[0:seg].reshape(cp, 2, cap, hidden)
        z1[step] = rows_in[seg:2 * seg].reshape(nx, 2, cap, hidden)
        for dc, dk in col_peers:
            target = device(dc, 0, dk)
            ret[0, step, dc, dk] = go(z0.at[step, target[1], (k + dk) % 2], b0.at[step, c, k], ret_y, (step, dc, dk), target)
        b0[step, c, k] = z0[step, c, k]
        for dx, dk in row_peers:
            target = device(0, dx, dk)
            ret[1, step, dx, dk] = go(z1.at[step, (x + dx) % nx, (k + dk) % 2], b1.at[step, x, k], ret_x, (step, dx, dk), target)
        b1[step, x, k] = z1[step, x, k]

    fin = {}
    for step in range(cp):
        back = order[step]
        for dc, dk in col_peers:
            ret[0, step, dc, dk].wait_recv()
        if step:
            fin[0, step] = go(b0.at[step], f0.at[x], fin_x, (step,), device(0, nx - back, 0))
        for dx, dk in row_peers:
            ret[1, step, dx, dk].wait_recv()
        if step:
            fin[1, step] = go(b1.at[step], f1.at[c], fin_y, (step,), device(cp - back, 0, 0))

    slot_f = slot_row.astype(jnp.float32)
    gates = [[jnp.transpose(jnp.broadcast_to(g_ref[b, i:i + 1, :], (tokens, tokens))) for i in range(2)] for b in range(2)]
    for step in range(cp):
        srcs = [(here[b] + order[step]) % size[b] for b in range(2)]
        picks = []
        for b in range(2):
            want = slot_f + (srcs[b] * seg).astype(jnp.float32)
            picks.append(jnp.concatenate([jnp.transpose(jnp.where(pos_ref[2 * b + i:2 * b + i + 1] == want, 1.0, 0.0)) for i in range(2)], axis=0).astype(jnp.bfloat16))
        if step:
            fin[0, step].wait_recv()
            fin[1, step].wait_recv()

        @pl.loop(0, hidden // 512)
        def _(n):
            at = pl.ds(pl.multiple_of(n * 512, 512), 512)
            for b in range(2):
                rows = (f0, f1)[b][srcs[b], :, :, :, at] if step else (b0, b1)[b][0, :, :, :, at]
                got = jnp.dot(picks[b], rows.reshape(seg, 512), preferred_element_type=jnp.float32)
                if step:
                    got += mixed[b, :, at]
                if step < cp - 1:
                    mixed[b, :, at] = got
                else:
                    g0_tile, g1_tile = (jnp.concatenate([g] * (512 // tokens), axis=1) for g in gates[b])
                    both = g0_tile * got[:tokens] + g1_tile * got[tokens:]
                    y_ref[b, :, at] = (h_ref[b, :, at].astype(jnp.float32) + both).astype(jnp.bfloat16)

    for copy in started:
        copy.wait_send()


def run_experts(mid_rows, route, gates, w_gate, w_up, w_down, cp, tp, cap):
    n_micro, tokens, hidden = mid_rows.shape
    ff = w_gate.shape[1]
    bf16 = jnp.bfloat16
    nx = tp // 2
    by_x, by_y = (cp, cp, 2, cap, hidden), (cp, nx, 2, cap, hidden)
    rows = 2 * (tp * cap)
    vmem = pl.BlockSpec(memory_space=pltpu.VMEM)
    any_spec = pl.BlockSpec(memory_space=pl.ANY)
    dma = pltpu.SemaphoreType.DMA
    return pl.pallas_call(
        functools.partial(expert_body, cp, tp, cap),
        out_shape=jax.ShapeDtypeStruct(mid_rows.shape, bf16),
        in_specs=[vmem] * 3 + [any_spec] * 3,
        out_specs=vmem,
        scratch_shapes=[pltpu.VMEM(s, jnp.float32) for s in ((8, tokens), (8, tokens), (nx, 8, tokens), (cp, 8, tokens))]
        + [pltpu.VMEM((nx, tokens, hidden), bf16), pltpu.VMEM((cp, tokens, hidden), bf16)]
        + [pltpu.VMEM(s, bf16) for s in (by_x, by_y) * 5]
        + [pltpu.VMEM((hidden, ff), bf16), pltpu.VMEM((hidden, ff), bf16), pltpu.VMEM((ff, hidden), bf16)]
        + [pltpu.VMEM((rows, hidden), bf16), pltpu.VMEM((rows, ff), bf16), pltpu.VMEM((n_micro, 2 * tokens, hidden), jnp.float32)]
        + [dma((3,)), dma((2, nx)), dma((2, cp)), dma((2, 6)), dma((2, 6)), dma((2, cp, cp, 2)), dma((2, cp, nx, 2)), dma((2, cp, cp, 2)), dma((2, cp, nx, 2)), dma((2, cp)), dma((2, cp))],
        compiler_params=pltpu.CompilerParams(collective_id=1, has_side_effects=True, vmem_limit_bytes=60 << 20),
        cost_estimate=pl.CostEstimate(flops=6 * 4 * rows * hidden * ff, bytes_accessed=6 * hidden * ff, transcendentals=0),
    )(mid_rows, route, gates, w_gate, w_up, w_down)


def solution(mesh):
    cp_size = mesh.shape['cp']
    tp_size = mesh.shape['tp']
    experts = cp_size * tp_size
    row_spec = P(None, ('data', 'cp', 'tp'), None)
    head_spec = P(None, 'tp', None)
    out_spec = P('tp', None, None)
    expert_spec = P(('cp', 'tp'), None, None)

    def device_step(act_in, route_ids, route_gates, w_query, w_key, w_value, w_out, w_gate, w_up, w_down):
        n_micro, tokens, hidden = act_in.shape
        heads, head_dim = w_query.shape[1], w_query.shape[2]
        mid_rows = run_front(act_in, w_query, w_key, w_value, w_out, cp_size, tp_size, heads)

        capacity = (4 * tokens) // experts
        route = jnp.transpose(route_ids, (0, 2, 1))
        gates = jnp.transpose(route_gates, (0, 2, 1))
        return run_experts(mid_rows, route, gates, w_gate[0], w_up[0], w_down[0], cp_size, tp_size, capacity)

    return jax.shard_map(device_step, mesh=mesh, in_specs=(row_spec, row_spec, row_spec, head_spec, head_spec, head_spec, out_spec, expert_spec, expert_spec, expert_spec), out_specs=row_spec, check_vma=False)
```

```python
import functools

import jax
import jax.numpy as jnp
from jax import lax
from jax.experimental import pallas as pl
from jax.experimental.pallas import tpu as pltpu
from jax.sharding import PartitionSpec as P

LOG2E = 1.4426950408889634


MESH_ID = pl.DeviceIdType.MESH


def front_body(cp, tp, heads, strip_len, x_hbm, wq_hbm, wk_hbm, wv_hbm, wo_hbm, h_ref, xg, wo, w, u, q_out, s_ref, o_st, o_rows,
               peaks, totals, accs, raw, a_sum, in_sem, x_sem, bulk_sem, strip_sem, lane_sem, mate_sem, u_sem, o_sem):
    d, c, t = lax.axis_index('data'), lax.axis_index('cp'), lax.axis_index('tp')
    nx = tp // 2
    x, k = t // 2, t % 2
    tokens, hidden = x_hbm.shape[1], x_hbm.shape[2]
    half_rows = tokens * tp
    pieces = 2 * cp
    piece_len = half_rows // 2
    head_dim = o_st.shape[1]
    width = 3 * head_dim
    left, right, far = ((x + nx - 1) % nx) * 2, ((x + 1) % nx) * 2, ((x + 2) % nx) * 2
    mine, other = k, 1 - k
    mate = 2 * x + other

    split = wo_hbm.shape[0] - strip_len * cp
    strip_rows = pl.ds(split + strip_len * c, strip_len)
    loads = [pltpu.make_async_copy(x_hbm, xg.at[t], in_sem.at[0]), pltpu.make_async_copy(wq_hbm, raw.at[0], in_sem.at[1]), pltpu.make_async_copy(wo_hbm.at[pl.ds(0, split)], wo.at[x, k, pl.ds(0, split)], in_sem.at[2]),
             pltpu.make_async_copy(wo_hbm.at[strip_rows], wo.at[x, k, strip_rows], in_sem.at[3]),
             pltpu.make_async_copy(wk_hbm, raw.at[1], in_sem.at[4]), pltpu.make_async_copy(wv_hbm, raw.at[2], in_sem.at[5])]
    for load in loads:
        load.start()
    barrier = pltpu.get_barrier_semaphore()
    peers = [(dc, dt) for dc in range(cp) for dt in range(tp) if dc or dt]
    for dc, dt in peers:
        pl.semaphore_signal(barrier, inc=1, device_id=(d, (c + dc) % cp, (t + dt) % tp), device_id_type=MESH_ID)
    pl.semaphore_wait(barrier, len(peers))

    def send(src, dst, sems, key, cc, tt):
        return pltpu.make_async_remote_copy(src_ref=src, dst_ref=dst, send_sem=sems.at[(0,) + key], recv_sem=sems.at[(1,) + key], device_id=(d, cc, tt), device_id_type=MESH_ID)

    names = ['r0', 'r1', 'r2', 'l0', 'l1', 'l2'] + ['p%d' % i for i in range(8)]

    def ring(view, sems, with_mate):
        sent = {}

        def start(name, src, part, target):
            if with_mate or name[0] != 'p':
                sent[name] = send(view(src, part), view(src, part), sems, (names.index(name),), c, target)
                sent[name].start()

        def wave(n):
            if n == 0:
                start('p0', t, 0, mate)
                start('p1', t, 1, mate)
                start('r0', t, 0, right + mine)
                start('l0', t, 1, left + mine)
                start('r1', t, 1, right + mine)
                start('l1', t, 0, left + mine)
            elif n == 1:
                sent['r0'].wait_recv()
                start('r2', left + mine, 0, right + mine)
                start('p2', left + mine, 0, mate)
                sent['l0'].wait_recv()
                start('l2', right + mine, 1, left + mine)
                start('p3', right + mine, 1, mate)
            elif n == 2:
                sent['r1'].wait_recv()
                start('p4', left + mine, 1, mate)
                sent['l1'].wait_recv()
                start('p5', right + mine, 0, mate)
            else:
                sent['r2'].wait_recv()
                start('p6', far + mine, 0, mate)
                sent['l2'].wait_recv()
                start('p7', far + mine, 1, mate)
        return sent, wave

    part_rows = split // 2

    def bulk(src, part):
        return wo.at[src // 2, src % 2, pl.ds(part * part_rows, part_rows)]

    def strip(src, part):
        return wo.at[src // 2, src % 2, pl.ds(split + strip_len * c, strip_len), pl.ds(part * (hidden // 2), hidden // 2)]

    def lane(q):
        return wo.at[:, k, pl.ds(split + strip_len * q, strip_len)]

    x_sent, x_wave = ring(lambda src, part: xg.at[src, part], x_sem, True)
    bulk_sent, bulk_wave = ring(bulk, bulk_sem, True)
    strip_sent, strip_wave = ring(strip, strip_sem, False)
    lane_y = {dc: send(lane(c), lane(c), lane_sem, (dc,), (c + dc) % cp, t) for dc in (1, cp - 1, 2)}
    lane_mate = {dc: send(lane((c + cp - dc) % cp), lane((c + cp - dc) % cp), mate_sem, (dc,), c, mate) for dc in (0, 1, cp - 1, 2)}

    def project(tt, s):
        @pl.loop(0, heads * width // 256)
        def _(n):
            at = pl.ds(pl.multiple_of(n * 256, 256), 256)
            q_out[tt, s, :, at] = jnp.dot(xg[tt, s], w[:, at], preferred_element_type=jnp.float32).astype(jnp.bfloat16)

        rows = pl.ds(pl.multiple_of(c * half_rows + tt * tokens, tokens), tokens)
        for dc in (1, cp - 1, 2):
            c2 = (c + dc) % cp
            lanes = pl.ds(pl.multiple_of(c2 % heads * width, 128), width)
            copy = send(q_out.at[tt, s, :, lanes], u.at[rows], u_sem, (dc, tt), c2, t)
            pl.when(c2 // heads == s)(copy.start)

        @pl.when(c // heads == s)
        def _():
            lanes = pl.ds(pl.multiple_of(c % heads * width, 128), width)
            u[rows] = q_out[tt, s, :, lanes]

    def relayout(j, load):
        load.wait()

        @pl.loop(0, hidden // 128)
        def _(i):
            at = pl.ds(pl.multiple_of(i * 128, 128), 128)
            flat = raw[j, at].reshape(128, heads * head_dim)
            for n in range(heads):
                w[at, n * width + j * head_dim:n * width + (j + 1) * head_dim] = flat[:, n * head_dim:(n + 1) * head_dim]

    loads[0].wait()
    x_wave(0)
    loads[3].wait()
    strip_wave(0)
    for j, i in enumerate((1, 4, 5)):
        relayout(j, loads[i])
    project(t, 0)
    project(t, 1)
    for s, name in ((0, 'p0'), (1, 'p1')):
        x_sent[name].wait_recv()
        project(mate, s)
    x_wave(1)
    project(left + mine, 0)
    project(right + mine, 1)
    x_sent['p2'].wait_recv()
    project(left + other, 0)
    x_sent['p3'].wait_recv()
    project(right + other, 1)
    x_wave(2)
    strip_wave(1)
    loads[2].wait()
    bulk_wave(0)
    project(left + mine, 1)
    project(right + mine, 0)
    x_sent['p4'].wait_recv()
    project(left + other, 1)
    x_sent['p5'].wait_recv()
    project(right + other, 0)
    x_wave(3)
    project(far + mine, 0)
    project(far + mine, 1)
    x_sent['p6'].wait_recv()
    project(far + other, 0)
    x_sent['p7'].wait_recv()
    project(far + other, 1)
    strip_wave(2)
    strip_wave(3)
    for dc in (1, cp - 1, 2):
        lane_y[dc].start()
    lane_mate[0].start()

    def u_copy(dc, tt):
        c2 = (c + dc) % cp
        lanes = pl.ds(pl.multiple_of(c2 % heads * width, 128), width)
        rows = pl.ds(pl.multiple_of(c * half_rows + tt * tokens, tokens), tokens)
        return send(q_out.at[tt, c2 // heads, :, lanes], u.at[rows], u_sem, (dc, tt), c2, t)

    for dc in (1, cp - 1, 2):
        for tt in range(tp):
            u_copy(dc, tt).wait_recv()
    bulk_wave(1)

    factor = head_dim ** -0.5 * LOG2E
    per_half = tp // 2

    def offset(n):
        return pl.multiple_of(jnp.where(n < cp, 2 * piece_len * n, 2 * piece_len * (pieces - 1 - n) + piece_len), piece_len)

    def fold(op, wide):
        parts = [wide[:, i * 128:(i + 1) * 128] for i in range(piece_len // 128)]
        while len(parts) > 1:
            parts = [op(a, b) for a, b in zip(parts[::2], parts[1::2])]
        return parts[0]

    row = lax.broadcasted_iota(jnp.int32, (piece_len, piece_len), 0)
    col = lax.broadcasted_iota(jnp.int32, (piece_len, piece_len), 1)
    unit_seq = c // heads
    unit_head = t * heads + c % heads

    def o_copy(rows, dcl, dtl, cc, tt):
        lanes = pl.ds(pl.multiple_of(unit_head * head_dim, 128), head_dim)
        return send(o_st.at[rows], o_rows.at[unit_seq, :, lanes], o_sem, (dcl, dtl), cc, tt)

    gap = col - row

    @pl.loop(0, cp)
    def _(turn):
        p = (c + 1 + turn) % cp
        lo, hi = p, pieces - 1 - p

        def place(j):
            if j >= cp:
                return hi, j - p - 1, 1
            is_lo = j <= p
            return jnp.where(is_lo, lo, hi), jnp.where(is_lo, j, j - p - 1), jnp.where(is_lo, 0, 1)

        def scores(j):
            piece, n, _ = place(j)
            q_rows = u[pl.ds(offset(piece), piece_len), 0:head_dim]
            k_rows = u[pl.ds(offset(n), piece_len), head_dim:2 * head_dim]
            s = lax.dot_general(q_rows, k_rows, (((1,), (1,)), ((), ())), preferred_element_type=jnp.float32)
            if j == pieces:
                s = jnp.where(gap <= 0, s, -jnp.inf)
            elif j < cp:
                s = jnp.where(gap <= jnp.where(j == p, 0, piece_len), s, -jnp.inf)
            s_ref[j] = s
            return fold(jnp.maximum, s)

        high = scores(cp)
        for j in range(cp + 1, pieces + 1):
            high = jnp.maximum(high, scores(j))
        peaks[1] = high
        peaks[0] = jnp.full_like(high, -jnp.inf)
        for j in range(cp):
            slot = place(j)[2]
            peaks[slot] = jnp.maximum(peaks[slot], scores(j))
        for slot in range(2):
            peaks[slot] = jnp.broadcast_to(jnp.max(peaks[slot], axis=1, keepdims=True) * factor, high.shape)

        def weigh(j):
            _, n, slot = place(j)
            peak = peaks[slot]
            s = s_ref[j]
            e = jnp.concatenate([jnp.exp2(s[:, i * 128:(i + 1) * 128] * factor - peak) for i in range(piece_len // 128)], axis=1)
            v_rows = u[pl.ds(offset(n), piece_len), 2 * head_dim:3 * head_dim]
            return fold(jnp.add, e), jnp.dot(e.astype(jnp.bfloat16), v_rows, preferred_element_type=jnp.float32)

        total, acc = weigh(cp)
        for j in range(cp + 1, pieces + 1):
            more, part = weigh(j)
            total, acc = total + more, acc + part
        totals[0], accs[0] = jnp.zeros_like(total), jnp.zeros_like(acc)
        totals[1], accs[1] = total, acc
        for j in range(cp):
            slot = place(j)[2]
            more, part = weigh(j)
            totals[slot] += more
            accs[slot] += part
        for slot, piece in enumerate((lo, hi)):
            o_st[pl.ds(offset(piece), piece_len), :] = (accs[slot] / jnp.sum(totals[slot], axis=1, keepdims=True)).astype(jnp.bfloat16)
        for i in range(2 * per_half):
            tt = (t + 1 + i) % tp
            rows = pl.ds(pl.multiple_of(p * 2 * piece_len + tt * tokens, tokens), tokens)
            dcl, dtl = (p - c + cp) % cp, (tt - t + tp) % tp
            pl.when(dcl + dtl > 0)(o_copy(rows, dcl, dtl, p, tt).start)

            @pl.when(dcl + dtl == 0)
            def _():
                lanes = pl.ds(pl.multiple_of(unit_head * head_dim, 128), head_dim)
                o_rows[unit_seq, :, lanes] = o_st[rows]

    for dc in (1, cp - 1, 2):
        lane_y[dc].wait_recv()
        lane_mate[dc].start()
    bulk_wave(2)
    first_rows = pl.ds(0, tokens)
    o_all = [o_copy(first_rows, dc, dt, (c + dc) % cp, (t + dt) % tp) for dc, dt in peers]
    per_chip = 2 * heads * head_dim

    def contract(dx, names):
        xs = (x + nx - dx) % nx
        for name in names:
            bulk_sent[name].wait_recv()
        for dc in range(cp):
            for dk in range(2):
                if dx or dc or dk:
                    dt = (t + tp - 2 * xs - (k + dk) % 2) % tp
                    o_copy(first_rows, dc, dt, (c + dc) % cp, (t + dt) % tp).wait_recv()

        @pl.loop(0, hidden // 512)
        def _(n):
            at = pl.ds(pl.multiple_of(n * 512, 512), 512)
            o_part = o_rows[:, :, pl.ds(pl.multiple_of(xs * per_chip, per_chip), per_chip)].reshape(2 * tokens, per_chip)
            a = jnp.dot(o_part, wo[xs, :, :, at].reshape(per_chip, 512), preferred_element_type=jnp.float32)
            if dx:
                a += a_sum[:, at]
            if dx == 2:
                h_ref[:, :, at] = (xg[t, :, :, at].astype(jnp.float32) + a.reshape(2, tokens, 512)).astype(jnp.bfloat16)
            else:
                a_sum[:, at] = a

    for copy in lane_mate.values():
        copy.wait_recv()
    contract(0, ('p0', 'p1'))
    bulk_wave(3)
    contract(1, ('p2', 'p4'))
    contract(nx - 1, ('p3', 'p5'))
    contract(2, ('p6', 'p7'))

    for copy in list(x_sent.values()) + list(bulk_sent.values()) + list(strip_sent.values()) + list(lane_y.values()) + list(lane_mate.values()) + o_all:
        copy.wait_send()
    for dc in (1, cp - 1, 2):
        for tt in range(tp):
            u_copy(dc, tt).wait_send()


def run_front(act_in, w_query, w_key, w_value, w_out, cp, tp, heads):
    n_micro, tokens, hidden = act_in.shape
    head_dim = w_out.shape[1]
    half_rows = tokens * tp
    rows = cp * half_rows
    bf16 = jnp.bfloat16
    any_spec = pl.BlockSpec(memory_space=pl.ANY)
    dma = pltpu.SemaphoreType.DMA
    vmem = [(tp, n_micro, tokens, hidden), (tp // 2, 2, heads * head_dim, hidden), (hidden, heads * 3 * head_dim), (rows, 3 * head_dim), (tp, n_micro, tokens, heads * 3 * head_dim)]
    piece = half_rows // 2
    return pl.pallas_call(
        functools.partial(front_body, cp, tp, heads, 16),
        out_shape=jax.ShapeDtypeStruct(act_in.shape, bf16),
        in_specs=[any_spec] * 5,
        out_specs=pl.BlockSpec(memory_space=pltpu.VMEM),
        scratch_shapes=[pltpu.VMEM(s, bf16) for s in vmem]
        + [pltpu.VMEM((2 * cp + 1, piece, piece), jnp.float32), pltpu.VMEM((rows, head_dim), bf16), pltpu.VMEM((n_micro, tokens, tp * heads * head_dim), bf16)]
        + [pltpu.VMEM((2, piece, 128), jnp.float32), pltpu.VMEM((2, piece, 128), jnp.float32), pltpu.VMEM((2, piece, head_dim), jnp.float32), pltpu.VMEM((3, hidden, heads, head_dim), bf16), pltpu.VMEM((n_micro * tokens, hidden), jnp.float32)]
        + [dma((6,)), dma((2, 14)), dma((2, 14)), dma((2, 14)), dma((2, cp)), dma((2, cp)), dma((2, cp, tp)), dma((2, cp, tp))],
        compiler_params=pltpu.CompilerParams(collective_id=2, has_side_effects=True, vmem_limit_bytes=56 << 20),
        cost_estimate=pl.CostEstimate(flops=8 * rows * hidden * head_dim * 3, bytes_accessed=20 << 20, transcendentals=0),
    )(act_in, w_query, w_key, w_value, w_out.reshape(heads * head_dim, hidden))


def expert_body(cp, tp, cap, h_ref, route_ref, g_ref, wg_hbm, wu_hbm, wd_hbm, y_ref,
                ids_ref, pos_ref, ids_x, ids_y, g0, g1, s0, s1, e0, e1, z0, z1, b0, b1, f0, f1, wg, wu, wd, rows_in, act, mixed, w_sem,
                idx_sem, idy_sem, ring_x, ring_y, hop_y, hop_x, ret_y, ret_x, fin_x, fin_y):
    d, c, t = lax.axis_index('data'), lax.axis_index('cp'), lax.axis_index('tp')
    tokens, hidden = h_ref.shape[1], h_ref.shape[2]
    ff = wg.shape[1]
    nx = tp // 2
    x, k = t // 2, t % 2
    order = sorted(range(cp), key=lambda i: min(i, cp - i))
    seg = tp * cap
    half = tokens // 2

    weights = [pltpu.make_async_copy(a, b, w_sem.at[i]) for i, (a, b) in enumerate(((wg_hbm, wg), (wu_hbm, wu), (wd_hbm, wd)))]
    for copy in weights:
        copy.start()

    def device(dc, dx, dk):
        return (d, (c + dc) % cp, ((x + dx) % nx) * 2 + (k + dk) % 2)

    row_peers = [(dx, dk) for dx in order for dk in (0, 1) if dx or dk]
    col_peers = [(dc, dk) for dc in order for dk in (0, 1) if dc or dk]
    barrier = pltpu.get_barrier_semaphore()
    peers = [(0, dx, dk) for dx, dk in row_peers] + [(dc, 0, dk) for dc, dk in col_peers if dc]
    for peer in peers:
        pl.semaphore_signal(barrier, inc=1, device_id=device(*peer), device_id_type=MESH_ID)
    experts = cp * tp
    expert = lax.broadcasted_iota(jnp.int32, (experts, tokens), 0)
    before = lax.broadcasted_iota(jnp.int32, (tokens, tokens), 0) < lax.broadcasted_iota(jnp.int32, (tokens, tokens), 1)
    before = jnp.where(before, 1.0, 0.0).astype(jnp.bfloat16)
    e_col, e_row = expert % tp, expert // tp
    bases = ((((e_col // 2 * cp + e_row) * 2 + e_col % 2) * cap).astype(jnp.float32), (expert * cap).astype(jnp.float32))
    ids_ref[...] = jnp.zeros_like(ids_ref)
    for b in range(2):
        used = jnp.zeros((experts, 1), jnp.float32)
        for i in range(2):
            row = 2 * b + i
            hit = jnp.where(expert == route_ref[b, i:i + 1, :], 1.0, 0.0)
            rank = jnp.dot(hit.astype(jnp.bfloat16), before, preferred_element_type=jnp.float32) + used
            used = used + jnp.sum(hit, axis=1, keepdims=True)
            ids_ref[row:row + 1] = jnp.sum(hit * (rank + bases[1]), axis=0, keepdims=True)
            pos_ref[row:row + 1] = jnp.sum(hit * (rank + bases[b]), axis=0, keepdims=True)
    pl.semaphore_wait(barrier, len(peers))

    def send(src, dst, sems, key, target):
        return pltpu.make_async_remote_copy(src_ref=src, dst_ref=dst, send_sem=sems.at[(0,) + key], recv_sem=sems.at[(1,) + key], device_id=target, device_id_type=MESH_ID)

    started = []

    def go(*args):
        copy = send(*args)
        copy.start()
        started.append(copy)
        return copy

    ids_sent = {}
    for i in order[1:]:
        ids_sent[0, i] = go(ids_ref, ids_x.at[x], idx_sem, (i,), device(0, i, 0))
        ids_sent[1, i] = go(ids_ref, ids_y.at[c], idy_sem, (i,), device(i, 0, 0))

    parts = (pl.ds(0, half), pl.ds(half, half))
    ahead = (device(0, 1, 0), device(1, 0, 0))
    behind = (device(0, nx - 1, 0), device(cp - 1, 0, 0))
    here, size = (x, c), (nx, cp)
    held, sems = (g0, g1), (ring_x, ring_y)
    ring = {}
    for b in range(2):
        ring[b, 'r0'] = go(h_ref.at[b, parts[0]], held[b].at[here[b], parts[0]], sems[b], (0,), ahead[b])
        ring[b, 'l0'] = go(h_ref.at[b, parts[1]], held[b].at[here[b], parts[1]], sems[b], (1,), behind[b])
        ring[b, 'r1'] = go(h_ref.at[b, parts[1]], held[b].at[here[b], parts[1]], sems[b], (2,), ahead[b])
        ring[b, 'l1'] = go(h_ref.at[b, parts[0]], held[b].at[here[b], parts[0]], sems[b], (3,), behind[b])

    def relay(b):
        prev, nxt = (here[b] + size[b] - 1) % size[b], (here[b] + 1) % size[b]
        ring[b, 'r0'].wait_recv()
        ring[b, 'r2'] = go(held[b].at[prev, parts[0]], held[b].at[prev, parts[0]], sems[b], (4,), ahead[b])
        ring[b, 'l0'].wait_recv()
        ring[b, 'l2'] = go(held[b].at[nxt, parts[1]], held[b].at[nxt, parts[1]], sems[b], (5,), behind[b])

    slot_row = lax.broadcasted_iota(jnp.int32, (seg, tokens), 0)
    group = 2 * cap
    wanted = ((slot_row // group * (tp * cap) + x * group + slot_row % group).astype(jnp.float32), (slot_row + c * seg).astype(jnp.float32))
    hop = {}

    def stage(b, step):
        back = order[step]
        src = (here[b] + size[b] - back) % size[b]
        out = (s0, s1)[b]
        if step:
            ids_sent[b, back].wait_recv()
            ids = (ids_x, ids_y)[b][src]
        else:
            ids = ids_ref[...]
        hit = (ids[2 * b:2 * b + 1] == wanted[b]) | (ids[2 * b + 1:2 * b + 2] == wanted[b])
        sel = jnp.where(hit, 1.0, 0.0).astype(jnp.bfloat16)

        @pl.loop(0, hidden // 512)
        def _(n):
            at = pl.ds(pl.multiple_of(n * 512, 512), 512)
            rows = held[b][src, :, at] if step else h_ref[b, :, at]
            got = jnp.dot(sel, rows, preferred_element_type=jnp.float32).astype(jnp.bfloat16)
            out[step, :, :, :, at] = got.reshape(out.shape[1:4] + (512,))

        if b == 0:
            for dc, dk in col_peers:
                target = device(dc, 0, dk)
                hop[0, step, dc, dk] = go(s0.at[step, target[1], (k + dk) % 2], e0.at[src, c, k], hop_y, (step, dc, dk), target)
            e0[src, c, k] = s0[step, c, k]
        else:
            for dx, dk in row_peers:
                target = device(0, dx, dk)
                hop[1, step, dx, dk] = go(s1.at[step, (x + dx) % nx, (k + dk) % 2], e1.at[src, x, k], hop_x, (step, dx, dk), target)
            e1[src, x, k] = s1[step, x, k]

    stage(0, 0)
    stage(1, 0)
    relay(0)
    relay(1)
    for b in range(2):
        ring[b, 'r1'].wait_recv()
        stage(b, 1)
    for b in range(2):
        ring[b, 'l1'].wait_recv()
        stage(b, 2)
    for b in range(2):
        ring[b, 'r2'].wait_recv()
        ring[b, 'l2'].wait_recv()
        stage(b, 3)
    for copy in weights:
        copy.wait()

    def hidden_tile(at, width):
        both = jnp.dot(rows_in[...], jnp.concatenate([wg[:, at], wu[:, at]], axis=1), preferred_element_type=jnp.float32)
        gate, up = both[:, :width], both[:, width:]
        act[:, at] = (jax.nn.silu(gate) * up).astype(jnp.bfloat16)

    def run_expert():
        @pl.loop(0, ff // 256)
        def _(n):
            hidden_tile(pl.ds(pl.multiple_of(n * 256, 256), 256), 256)

        if ff % 256:
            hidden_tile(pl.ds(ff // 256 * 256, ff % 256), ff % 256)

        @pl.loop(0, hidden // 512)
        def _(n):
            at = pl.ds(pl.multiple_of(n * 512, 512), 512)
            rows_in[:, at] = jnp.dot(act[...], wd[:, at], preferred_element_type=jnp.float32).astype(jnp.bfloat16)

    ret = {}
    for step in range(cp):
        xs, cs = (x + nx - order[step]) % nx, (c + cp - order[step]) % cp
        for dc, dk in col_peers:
            hop[0, step, dc, dk].wait_recv()
        for dx, dk in row_peers:
            hop[1, step, dx, dk].wait_recv()
        rows_in[0:seg] = e0[xs].reshape(seg, hidden)
        rows_in[seg:2 * seg] = e1[cs].reshape(seg, hidden)
        run_expert()
        z0[step] = rows_in[0:seg].reshape(cp, 2, cap, hidden)
        z1[step] = rows_in[seg:2 * seg].reshape(nx, 2, cap, hidden)
        for dc, dk in col_peers:
            target = device(dc, 0, dk)
            ret[0, step, dc, dk] = go(z0.at[step, target[1], (k + dk) % 2], b0.at[step, c, k], ret_y, (step, dc, dk), target)
        b0[step, c, k] = z0[step, c, k]
        for dx, dk in row_peers:
            target = device(0, dx, dk)
            ret[1, step, dx, dk] = go(z1.at[step, (x + dx) % nx, (k + dk) % 2], b1.at[step, x, k], ret_x, (step, dx, dk), target)
        b1[step, x, k] = z1[step, x, k]

    fin = {}
    for step in range(cp):
        back = order[step]
        for dc, dk in col_peers:
            ret[0, step, dc, dk].wait_recv()
        if step:
            fin[0, step] = go(b0.at[step], f0.at[x], fin_x, (step,), device(0, nx - back, 0))
        for dx, dk in row_peers:
            ret[1, step, dx, dk].wait_recv()
        if step:
            fin[1, step] = go(b1.at[step], f1.at[c], fin_y, (step,), device(cp - back, 0, 0))

    slot_f = slot_row.astype(jnp.float32)
    gates = [[jnp.transpose(jnp.broadcast_to(g_ref[b, i:i + 1, :], (tokens, tokens))) for i in range(2)] for b in range(2)]
    for step in range(cp):
        srcs = [(here[b] + order[step]) % size[b] for b in range(2)]
        picks = []
        for b in range(2):
            want = slot_f + (srcs[b] * seg).astype(jnp.float32)
            picks.append(jnp.concatenate([jnp.transpose(jnp.where(pos_ref[2 * b + i:2 * b + i + 1] == want, 1.0, 0.0)) for i in range(2)], axis=0).astype(jnp.bfloat16))
        if step:
            fin[0, step].wait_recv()
            fin[1, step].wait_recv()

        @pl.loop(0, hidden // 512)
        def _(n):
            at = pl.ds(pl.multiple_of(n * 512, 512), 512)
            for b in range(2):
                rows = (f0, f1)[b][srcs[b], :, :, :, at] if step else (b0, b1)[b][0, :, :, :, at]
                got = jnp.dot(picks[b], rows.reshape(seg, 512), preferred_element_type=jnp.float32)
                if step:
                    got += mixed[b, :, at]
                if step < cp - 1:
                    mixed[b, :, at] = got
                else:
                    g0_tile, g1_tile = (jnp.concatenate([g] * (512 // tokens), axis=1) for g in gates[b])
                    both = g0_tile * got[:tokens] + g1_tile * got[tokens:]
                    y_ref[b, :, at] = (h_ref[b, :, at].astype(jnp.float32) + both).astype(jnp.bfloat16)

    for copy in started:
        copy.wait_send()


def run_experts(mid_rows, route, gates, w_gate, w_up, w_down, cp, tp, cap):
    n_micro, tokens, hidden = mid_rows.shape
    ff = w_gate.shape[1]
    bf16 = jnp.bfloat16
    nx = tp // 2
    by_x, by_y = (cp, cp, 2, cap, hidden), (cp, nx, 2, cap, hidden)
    rows = 2 * (tp * cap)
    vmem = pl.BlockSpec(memory_space=pltpu.VMEM)
    any_spec = pl.BlockSpec(memory_space=pl.ANY)
    dma = pltpu.SemaphoreType.DMA
    return pl.pallas_call(
        functools.partial(expert_body, cp, tp, cap),
        out_shape=jax.ShapeDtypeStruct(mid_rows.shape, bf16),
        in_specs=[vmem] * 3 + [any_spec] * 3,
        out_specs=vmem,
        scratch_shapes=[pltpu.VMEM(s, jnp.float32) for s in ((8, tokens), (8, tokens), (nx, 8, tokens), (cp, 8, tokens))]
        + [pltpu.VMEM((nx, tokens, hidden), bf16), pltpu.VMEM((cp, tokens, hidden), bf16)]
        + [pltpu.VMEM(s, bf16) for s in (by_x, by_y) * 5]
        + [pltpu.VMEM((hidden, ff), bf16), pltpu.VMEM((hidden, ff), bf16), pltpu.VMEM((ff, hidden), bf16)]
        + [pltpu.VMEM((rows, hidden), bf16), pltpu.VMEM((rows, ff), bf16), pltpu.VMEM((n_micro, 2 * tokens, hidden), jnp.float32)]
        + [dma((3,)), dma((2, nx)), dma((2, cp)), dma((2, 6)), dma((2, 6)), dma((2, cp, cp, 2)), dma((2, cp, nx, 2)), dma((2, cp, cp, 2)), dma((2, cp, nx, 2)), dma((2, cp)), dma((2, cp))],
        compiler_params=pltpu.CompilerParams(collective_id=1, has_side_effects=True, vmem_limit_bytes=60 << 20),
        cost_estimate=pl.CostEstimate(flops=6 * 4 * rows * hidden * ff, bytes_accessed=6 * hidden * ff, transcendentals=0),
    )(mid_rows, route, gates, w_gate, w_up, w_down)


def solution(mesh):
    cp_size = mesh.shape['cp']
    tp_size = mesh.shape['tp']
    experts = cp_size * tp_size
    row_spec = P(None, ('data', 'cp', 'tp'), None)
    head_spec = P(None, 'tp', None)
    out_spec = P('tp', None, None)
    expert_spec = P(('cp', 'tp'), None, None)

    def device_step(act_in, route_ids, route_gates, w_query, w_key, w_value, w_out, w_gate, w_up, w_down):
        n_micro, tokens, hidden = act_in.shape
        heads, head_dim = w_query.shape[1], w_query.shape[2]
        mid_rows = run_front(act_in, w_query, w_key, w_value, w_out, cp_size, tp_size, heads)

        capacity = (4 * tokens) // experts
        route = jnp.transpose(route_ids, (0, 2, 1))
        gates = jnp.transpose(route_gates, (0, 2, 1))
        return run_experts(mid_rows, route, gates, w_gate[0], w_up[0], w_down[0], cp_size, tp_size, capacity)

    return jax.shard_map(device_step, mesh=mesh, in_specs=(row_spec, row_spec, row_spec, head_spec, head_spec, head_spec, out_spec, expert_spec, expert_spec, expert_spec), out_specs=row_spec, check_vma=False)
```

```python
import functools

import jax
import jax.numpy as jnp
from jax import lax
from jax.experimental import pallas as pl
from jax.experimental.pallas import tpu as pltpu
from jax.sharding import PartitionSpec as P

LOG2E = 1.4426950408889634


MESH_ID = pl.DeviceIdType.MESH


def front_body(cp, tp, heads, strip_len, x_hbm, wq_hbm, wk_hbm, wv_hbm, wo_hbm, h_ref, xg, wo, w, u, q_out, s_ref, o_st, o_rows,
               peaks, totals, accs, raw, a_sum, in_sem, x_sem, bulk_sem, strip_sem, lane_sem, mate_sem, u_sem, o_sem):
    d, c, t = lax.axis_index('data'), lax.axis_index('cp'), lax.axis_index('tp')
    nx = tp // 2
    x, k = t // 2, t % 2
    tokens, hidden = x_hbm.shape[1], x_hbm.shape[2]
    half_rows = tokens * tp
    pieces = 2 * cp
    piece_len = half_rows // 2
    head_dim = o_st.shape[1]
    width = 3 * head_dim
    left, right, far = ((x + nx - 1) % nx) * 2, ((x + 1) % nx) * 2, ((x + 2) % nx) * 2
    mine, other = k, 1 - k
    mate = 2 * x + other

    split = wo_hbm.shape[0] - strip_len * cp
    strip_rows = pl.ds(split + strip_len * c, strip_len)
    loads = [pltpu.make_async_copy(x_hbm, xg.at[t], in_sem.at[0]), pltpu.make_async_copy(wq_hbm, raw.at[0], in_sem.at[1]), pltpu.make_async_copy(wo_hbm.at[pl.ds(0, split)], wo.at[x, k, pl.ds(0, split)], in_sem.at[2]),
             pltpu.make_async_copy(wo_hbm.at[strip_rows], wo.at[x, k, strip_rows], in_sem.at[3]),
             pltpu.make_async_copy(wk_hbm, raw.at[1], in_sem.at[4]), pltpu.make_async_copy(wv_hbm, raw.at[2], in_sem.at[5])]
    for load in loads:
        load.start()
    barrier = pltpu.get_barrier_semaphore()
    peers = [(dc, dt) for dc in range(cp) for dt in range(tp) if dc or dt]
    for dc, dt in peers:
        pl.semaphore_signal(barrier, inc=1, device_id=(d, (c + dc) % cp, (t + dt) % tp), device_id_type=MESH_ID)
    pl.semaphore_wait(barrier, len(peers))

    def send(src, dst, sems, key, cc, tt):
        return pltpu.make_async_remote_copy(src_ref=src, dst_ref=dst, send_sem=sems.at[(0,) + key], recv_sem=sems.at[(1,) + key], device_id=(d, cc, tt), device_id_type=MESH_ID)

    names = ['r0', 'r1', 'r2', 'l0', 'l1', 'l2'] + ['p%d' % i for i in range(8)]

    def ring(view, sems, with_mate):
        sent = {}

        def start(name, src, part, target):
            if with_mate or name[0] != 'p':
                sent[name] = send(view(src, part), view(src, part), sems, (names.index(name),), c, target)
                sent[name].start()

        def wave(n):
            if n == 0:
                start('p0', t, 0, mate)
                start('p1', t, 1, mate)
                start('r0', t, 0, right + mine)
                start('l0', t, 1, left + mine)
                start('r1', t, 1, right + mine)
                start('l1', t, 0, left + mine)
            elif n == 1:
                sent['r0'].wait_recv()
                start('r2', left + mine, 0, right + mine)
                start('p2', left + mine, 0, mate)
                sent['l0'].wait_recv()
                start('l2', right + mine, 1, left + mine)
                start('p3', right + mine, 1, mate)
            elif n == 2:
                sent['r1'].wait_recv()
                start('p4', left + mine, 1, mate)
                sent['l1'].wait_recv()
                start('p5', right + mine, 0, mate)
            else:
                sent['r2'].wait_recv()
                start('p6', far + mine, 0, mate)
                sent['l2'].wait_recv()
                start('p7', far + mine, 1, mate)
        return sent, wave

    part_rows = split // 2

    def bulk(src, part):
        return wo.at[src // 2, src % 2, pl.ds(part * part_rows, part_rows)]

    def strip(src, part):
        return wo.at[src // 2, src % 2, pl.ds(split + strip_len * c, strip_len), pl.ds(part * (hidden // 2), hidden // 2)]

    def lane(q):
        return wo.at[:, k, pl.ds(split + strip_len * q, strip_len)]

    x_sent, x_wave = ring(lambda src, part: xg.at[src, part], x_sem, True)
    bulk_sent, bulk_wave = ring(bulk, bulk_sem, True)
    strip_sent, strip_wave = ring(strip, strip_sem, False)
    lane_y = {dc: send(lane(c), lane(c), lane_sem, (dc,), (c + dc) % cp, t) for dc in (1, cp - 1, 2)}
    lane_mate = {dc: send(lane((c + cp - dc) % cp), lane((c + cp - dc) % cp), mate_sem, (dc,), c, mate) for dc in (0, 1, cp - 1, 2)}

    def project(tt, s):
        @pl.loop(0, heads * width // 256)
        def _(n):
            at = pl.ds(pl.multiple_of(n * 256, 256), 256)
            q_out[tt, s, :, at] = jnp.dot(xg[tt, s], w[:, at], preferred_element_type=jnp.float32).astype(jnp.bfloat16)

        rows = pl.ds(pl.multiple_of(c * half_rows + tt * tokens, tokens), tokens)
        for dc in (1, cp - 1, 2):
            c2 = (c + dc) % cp
            lanes = pl.ds(pl.multiple_of(c2 % heads * width, 128), width)
            copy = send(q_out.at[tt, s, :, lanes], u.at[rows], u_sem, (dc, tt), c2, t)
            pl.when(c2 // heads == s)(copy.start)

        @pl.when(c // heads == s)
        def _():
            lanes = pl.ds(pl.multiple_of(c % heads * width, 128), width)
            u[rows] = q_out[tt, s, :, lanes]

    def relayout(j, load):
        load.wait()

        @pl.loop(0, hidden // 128)
        def _(i):
            at = pl.ds(pl.multiple_of(i * 128, 128), 128)
            flat = raw[j, at].reshape(128, heads * head_dim)
            for n in range(heads):
                w[at, n * width + j * head_dim:n * width + (j + 1) * head_dim] = flat[:, n * head_dim:(n + 1) * head_dim]

    loads[0].wait()
    x_wave(0)
    loads[3].wait()
    strip_wave(0)
    for j, i in enumerate((1, 4, 5)):
        relayout(j, loads[i])
    odd = c % 2

    def either(one, two):
        project(jnp.where(odd == 0, one[0], two[0]), jnp.where(odd == 0, one[1], two[1]))
        project(jnp.where(odd == 0, two[0], one[0]), jnp.where(odd == 0, two[1], one[1]))

    either((t, 0), (t, 1))
    x_sent['p0'].wait_recv()
    x_sent['p1'].wait_recv()
    either((mate, 0), (mate, 1))
    x_wave(1)
    either((left + mine, 0), (right + mine, 1))
    x_sent['p2'].wait_recv()
    x_sent['p3'].wait_recv()
    either((left + other, 0), (right + other, 1))
    x_wave(2)
    strip_wave(1)
    loads[2].wait()
    bulk_wave(0)
    either((left + mine, 1), (right + mine, 0))
    x_sent['p4'].wait_recv()
    x_sent['p5'].wait_recv()
    either((left + other, 1), (right + other, 0))
    x_wave(3)
    either((far + mine, 0), (far + mine, 1))
    x_sent['p6'].wait_recv()
    x_sent['p7'].wait_recv()
    either((far + other, 0), (far + other, 1))
    strip_wave(2)
    strip_wave(3)
    for dc in (1, cp - 1, 2):
        lane_y[dc].start()
    lane_mate[0].start()

    def u_copy(dc, tt):
        c2 = (c + dc) % cp
        lanes = pl.ds(pl.multiple_of(c2 % heads * width, 128), width)
        rows = pl.ds(pl.multiple_of(c * half_rows + tt * tokens, tokens), tokens)
        return send(q_out.at[tt, c2 // heads, :, lanes], u.at[rows], u_sem, (dc, tt), c2, t)

    for dc in (1, cp - 1, 2):
        for tt in range(tp):
            u_copy(dc, tt).wait_recv()
    bulk_wave(1)

    factor = head_dim ** -0.5 * LOG2E
    per_half = tp // 2

    def offset(n):
        return pl.multiple_of(jnp.where(n < cp, 2 * piece_len * n, 2 * piece_len * (pieces - 1 - n) + piece_len), piece_len)

    def fold(op, wide):
        parts = [wide[:, i * 128:(i + 1) * 128] for i in range(piece_len // 128)]
        while len(parts) > 1:
            parts = [op(a, b) for a, b in zip(parts[::2], parts[1::2])]
        return parts[0]

    row = lax.broadcasted_iota(jnp.int32, (piece_len, piece_len), 0)
    col = lax.broadcasted_iota(jnp.int32, (piece_len, piece_len), 1)
    unit_seq = c // heads
    unit_head = t * heads + c % heads

    def o_copy(rows, dcl, dtl, cc, tt):
        lanes = pl.ds(pl.multiple_of(unit_head * head_dim, 128), head_dim)
        return send(o_st.at[rows], o_rows.at[unit_seq, :, lanes], o_sem, (dcl, dtl), cc, tt)

    gap = col - row

    @pl.loop(0, cp)
    def _(turn):
        p = (c + 1 + turn) % cp
        lo, hi = p, pieces - 1 - p

        def place(j):
            if j >= cp:
                return hi, j - p - 1, 1
            is_lo = j <= p
            return jnp.where(is_lo, lo, hi), jnp.where(is_lo, j, j - p - 1), jnp.where(is_lo, 0, 1)

        def scores(j):
            piece, n, _ = place(j)
            q_rows = u[pl.ds(offset(piece), piece_len), 0:head_dim]
            k_rows = u[pl.ds(offset(n), piece_len), head_dim:2 * head_dim]
            s = lax.dot_general(q_rows, k_rows, (((1,), (1,)), ((), ())), preferred_element_type=jnp.float32)
            if j == pieces:
                s = jnp.where(gap <= 0, s, -jnp.inf)
            elif j < cp:
                s = jnp.where(gap <= jnp.where(j == p, 0, piece_len), s, -jnp.inf)
            s_ref[j] = s
            return fold(jnp.maximum, s)

        high = scores(cp)
        for j in range(cp + 1, pieces + 1):
            high = jnp.maximum(high, scores(j))
        peaks[1] = high
        peaks[0] = jnp.full_like(high, -jnp.inf)
        for j in range(cp):
            slot = place(j)[2]
            peaks[slot] = jnp.maximum(peaks[slot], scores(j))
        for slot in range(2):
            peaks[slot] = jnp.broadcast_to(jnp.max(peaks[slot], axis=1, keepdims=True) * factor, high.shape)

        def weigh(j):
            _, n, slot = place(j)
            peak = peaks[slot]
            s = s_ref[j]
            e = jnp.concatenate([jnp.exp2(s[:, i * 128:(i + 1) * 128] * factor - peak) for i in range(piece_len // 128)], axis=1)
            v_rows = u[pl.ds(offset(n), piece_len), 2 * head_dim:3 * head_dim]
            return fold(jnp.add, e), jnp.dot(e.astype(jnp.bfloat16), v_rows, preferred_element_type=jnp.float32)

        total, acc = weigh(cp)
        for j in range(cp + 1, pieces + 1):
            more, part = weigh(j)
            total, acc = total + more, acc + part
        totals[0], accs[0] = jnp.zeros_like(total), jnp.zeros_like(acc)
        totals[1], accs[1] = total, acc
        for j in range(cp):
            slot = place(j)[2]
            more, part = weigh(j)
            totals[slot] += more
            accs[slot] += part
        for slot, piece in enumerate((lo, hi)):
            o_st[pl.ds(offset(piece), piece_len), :] = (accs[slot] / jnp.sum(totals[slot], axis=1, keepdims=True)).astype(jnp.bfloat16)
        for i in range(2 * per_half):
            tt = (t + 1 + i) % tp
            rows = pl.ds(pl.multiple_of(p * 2 * piece_len + tt * tokens, tokens), tokens)
            dcl, dtl = (p - c + cp) % cp, (tt - t + tp) % tp
            pl.when(dcl + dtl > 0)(o_copy(rows, dcl, dtl, p, tt).start)

            @pl.when(dcl + dtl == 0)
            def _():
                lanes = pl.ds(pl.multiple_of(unit_head * head_dim, 128), head_dim)
                o_rows[unit_seq, :, lanes] = o_st[rows]

    for dc in (1, cp - 1, 2):
        lane_y[dc].wait_recv()
        lane_mate[dc].start()
    bulk_wave(2)
    first_rows = pl.ds(0, tokens)
    o_all = [o_copy(first_rows, dc, dt, (c + dc) % cp, (t + dt) % tp) for dc, dt in peers]
    per_chip = 2 * heads * head_dim

    def contract(dx, names):
        xs = (x + nx - dx) % nx
        for name in names:
            bulk_sent[name].wait_recv()
        for dc in range(cp):
            for dk in range(2):
                if dx or dc or dk:
                    dt = (t + tp - 2 * xs - (k + dk) % 2) % tp
                    o_copy(first_rows, dc, dt, (c + dc) % cp, (t + dt) % tp).wait_recv()

        @pl.loop(0, hidden // 512)
        def _(n):
            at = pl.ds(pl.multiple_of(n * 512, 512), 512)
            o_part = o_rows[:, :, pl.ds(pl.multiple_of(xs * per_chip, per_chip), per_chip)].reshape(2 * tokens, per_chip)
            a = jnp.dot(o_part, wo[xs, :, :, at].reshape(per_chip, 512), preferred_element_type=jnp.float32)
            if dx:
                a += a_sum[:, at]
            if dx == 2:
                h_ref[:, :, at] = (xg[t, :, :, at].astype(jnp.float32) + a.reshape(2, tokens, 512)).astype(jnp.bfloat16)
            else:
                a_sum[:, at] = a

    for copy in lane_mate.values():
        copy.wait_recv()
    contract(0, ('p0', 'p1'))
    bulk_wave(3)
    contract(1, ('p2', 'p4'))
    contract(nx - 1, ('p3', 'p5'))
    contract(2, ('p6', 'p7'))

    for copy in list(x_sent.values()) + list(bulk_sent.values()) + list(strip_sent.values()) + list(lane_y.values()) + list(lane_mate.values()) + o_all:
        copy.wait_send()
    for dc in (1, cp - 1, 2):
        for tt in range(tp):
            u_copy(dc, tt).wait_send()


def run_front(act_in, w_query, w_key, w_value, w_out, cp, tp, heads):
    n_micro, tokens, hidden = act_in.shape
    head_dim = w_out.shape[1]
    half_rows = tokens * tp
    rows = cp * half_rows
    bf16 = jnp.bfloat16
    any_spec = pl.BlockSpec(memory_space=pl.ANY)
    dma = pltpu.SemaphoreType.DMA
    vmem = [(tp, n_micro, tokens, hidden), (tp // 2, 2, heads * head_dim, hidden), (hidden, heads * 3 * head_dim), (rows, 3 * head_dim), (tp, n_micro, tokens, heads * 3 * head_dim)]
    piece = half_rows // 2
    return pl.pallas_call(
        functools.partial(front_body, cp, tp, heads, 16),
        out_shape=jax.ShapeDtypeStruct(act_in.shape, bf16),
        in_specs=[any_spec] * 5,
        out_specs=pl.BlockSpec(memory_space=pltpu.VMEM),
        scratch_shapes=[pltpu.VMEM(s, bf16) for s in vmem]
        + [pltpu.VMEM((2 * cp + 1, piece, piece), jnp.float32), pltpu.VMEM((rows, head_dim), bf16), pltpu.VMEM((n_micro, tokens, tp * heads * head_dim), bf16)]
        + [pltpu.VMEM((2, piece, 128), jnp.float32), pltpu.VMEM((2, piece, 128), jnp.float32), pltpu.VMEM((2, piece, head_dim), jnp.float32), pltpu.VMEM((3, hidden, heads, head_dim), bf16), pltpu.VMEM((n_micro * tokens, hidden), jnp.float32)]
        + [dma((6,)), dma((2, 14)), dma((2, 14)), dma((2, 14)), dma((2, cp)), dma((2, cp)), dma((2, cp, tp)), dma((2, cp, tp))],
        compiler_params=pltpu.CompilerParams(collective_id=2, has_side_effects=True, vmem_limit_bytes=56 << 20),
        cost_estimate=pl.CostEstimate(flops=8 * rows * hidden * head_dim * 3, bytes_accessed=20 << 20, transcendentals=0),
    )(act_in, w_query, w_key, w_value, w_out.reshape(heads * head_dim, hidden))


def expert_body(cp, tp, cap, h_ref, route_ref, g_ref, wg_hbm, wu_hbm, wd_hbm, y_ref,
                ids_ref, pos_ref, ids_x, ids_y, g0, g1, s0, s1, e0, e1, z0, z1, b0, b1, f0, f1, wg, wu, wd, rows_in, act, mixed, w_sem,
                idx_sem, idy_sem, ring_x, ring_y, hop_y, hop_x, ret_y, ret_x, fin_x, fin_y):
    d, c, t = lax.axis_index('data'), lax.axis_index('cp'), lax.axis_index('tp')
    tokens, hidden = h_ref.shape[1], h_ref.shape[2]
    ff = wg.shape[1]
    nx = tp // 2
    x, k = t // 2, t % 2
    order = sorted(range(cp), key=lambda i: min(i, cp - i))
    seg = tp * cap
    half = tokens // 2

    weights = [pltpu.make_async_copy(a, b, w_sem.at[i]) for i, (a, b) in enumerate(((wg_hbm, wg), (wu_hbm, wu), (wd_hbm, wd)))]
    for copy in weights:
        copy.start()

    def device(dc, dx, dk):
        return (d, (c + dc) % cp, ((x + dx) % nx) * 2 + (k + dk) % 2)

    row_peers = [(dx, dk) for dx in order for dk in (0, 1) if dx or dk]
    col_peers = [(dc, dk) for dc in order for dk in (0, 1) if dc or dk]
    barrier = pltpu.get_barrier_semaphore()
    peers = [(0, dx, dk) for dx, dk in row_peers] + [(dc, 0, dk) for dc, dk in col_peers if dc]
    for peer in peers:
        pl.semaphore_signal(barrier, inc=1, device_id=device(*peer), device_id_type=MESH_ID)
    experts = cp * tp
    expert = lax.broadcasted_iota(jnp.int32, (experts, tokens), 0)
    before = lax.broadcasted_iota(jnp.int32, (tokens, tokens), 0) < lax.broadcasted_iota(jnp.int32, (tokens, tokens), 1)
    before = jnp.where(before, 1.0, 0.0).astype(jnp.bfloat16)
    e_col, e_row = expert % tp, expert // tp
    bases = ((((e_col // 2 * cp + e_row) * 2 + e_col % 2) * cap).astype(jnp.float32), (expert * cap).astype(jnp.float32))
    ids_ref[...] = jnp.zeros_like(ids_ref)
    for b in range(2):
        used = jnp.zeros((experts, 1), jnp.float32)
        for i in range(2):
            row = 2 * b + i
            hit = jnp.where(expert == route_ref[b, i:i + 1, :], 1.0, 0.0)
            rank = jnp.dot(hit.astype(jnp.bfloat16), before, preferred_element_type=jnp.float32) + used
            used = used + jnp.sum(hit, axis=1, keepdims=True)
            ids_ref[row:row + 1] = jnp.sum(hit * (rank + bases[1]), axis=0, keepdims=True)
            pos_ref[row:row + 1] = jnp.sum(hit * (rank + bases[b]), axis=0, keepdims=True)
    pl.semaphore_wait(barrier, len(peers))

    def send(src, dst, sems, key, target):
        return pltpu.make_async_remote_copy(src_ref=src, dst_ref=dst, send_sem=sems.at[(0,) + key], recv_sem=sems.at[(1,) + key], device_id=target, device_id_type=MESH_ID)

    started = []

    def go(*args):
        copy = send(*args)
        copy.start()
        started.append(copy)
        return copy

    ids_sent = {}
    for i in order[1:]:
        ids_sent[0, i] = go(ids_ref, ids_x.at[x], idx_sem, (i,), device(0, i, 0))
        ids_sent[1, i] = go(ids_ref, ids_y.at[c], idy_sem, (i,), device(i, 0, 0))

    parts = (pl.ds(0, half), pl.ds(half, half))
    ahead = (device(0, 1, 0), device(1, 0, 0))
    behind = (device(0, nx - 1, 0), device(cp - 1, 0, 0))
    here, size = (x, c), (nx, cp)
    held, sems = (g0, g1), (ring_x, ring_y)
    ring = {}
    for b in range(2):
        ring[b, 'r0'] = go(h_ref.at[b, parts[0]], held[b].at[here[b], parts[0]], sems[b], (0,), ahead[b])
        ring[b, 'l0'] = go(h_ref.at[b, parts[1]], held[b].at[here[b], parts[1]], sems[b], (1,), behind[b])
        ring[b, 'r1'] = go(h_ref.at[b, parts[1]], held[b].at[here[b], parts[1]], sems[b], (2,), ahead[b])
        ring[b, 'l1'] = go(h_ref.at[b, parts[0]], held[b].at[here[b], parts[0]], sems[b], (3,), behind[b])

    def relay(b):
        prev, nxt = (here[b] + size[b] - 1) % size[b], (here[b] + 1) % size[b]
        ring[b, 'r0'].wait_recv()
        ring[b, 'r2'] = go(held[b].at[prev, parts[0]], held[b].at[prev, parts[0]], sems[b], (4,), ahead[b])
        ring[b, 'l0'].wait_recv()
        ring[b, 'l2'] = go(held[b].at[nxt, parts[1]], held[b].at[nxt, parts[1]], sems[b], (5,), behind[b])

    slot_row = lax.broadcasted_iota(jnp.int32, (seg, tokens), 0)
    group = 2 * cap
    wanted = ((slot_row // group * (tp * cap) + x * group + slot_row % group).astype(jnp.float32), (slot_row + c * seg).astype(jnp.float32))
    hop = {}

    def stage(b, step):
        back = order[step]
        src = (here[b] + size[b] - back) % size[b]
        out = (s0, s1)[b]
        if step:
            ids_sent[b, back].wait_recv()
            ids = (ids_x, ids_y)[b][src]
        else:
            ids = ids_ref[...]
        hit = (ids[2 * b:2 * b + 1] == wanted[b]) | (ids[2 * b + 1:2 * b + 2] == wanted[b])
        sel = jnp.where(hit, 1.0, 0.0).astype(jnp.bfloat16)

        @pl.loop(0, hidden // 512)
        def _(n):
            at = pl.ds(pl.multiple_of(n * 512, 512), 512)
            rows = held[b][src, :, at] if step else h_ref[b, :, at]
            got = jnp.dot(sel, rows, preferred_element_type=jnp.float32).astype(jnp.bfloat16)
            out[step, :, :, :, at] = got.reshape(out.shape[1:4] + (512,))

        if b == 0:
            for dc, dk in col_peers:
                target = device(dc, 0, dk)
                hop[0, step, dc, dk] = go(s0.at[step, target[1], (k + dk) % 2], e0.at[src, c, k], hop_y, (step, dc, dk), target)
            e0[src, c, k] = s0[step, c, k]
        else:
            for dx, dk in row_peers:
                target = device(0, dx, dk)
                hop[1, step, dx, dk] = go(s1.at[step, (x + dx) % nx, (k + dk) % 2], e1.at[src, x, k], hop_x, (step, dx, dk), target)
            e1[src, x, k] = s1[step, x, k]

    stage(0, 0)
    stage(1, 0)
    relay(0)
    relay(1)
    for b in range(2):
        ring[b, 'r1'].wait_recv()
        stage(b, 1)
    for b in range(2):
        ring[b, 'l1'].wait_recv()
        stage(b, 2)
    for b in range(2):
        ring[b, 'r2'].wait_recv()
        ring[b, 'l2'].wait_recv()
        stage(b, 3)
    for copy in weights:
        copy.wait()

    def hidden_tile(at, width):
        both = jnp.dot(rows_in[...], jnp.concatenate([wg[:, at], wu[:, at]], axis=1), preferred_element_type=jnp.float32)
        gate, up = both[:, :width], both[:, width:]
        act[:, at] = (jax.nn.silu(gate) * up).astype(jnp.bfloat16)

    def run_expert():
        @pl.loop(0, ff // 256)
        def _(n):
            hidden_tile(pl.ds(pl.multiple_of(n * 256, 256), 256), 256)

        if ff % 256:
            hidden_tile(pl.ds(ff // 256 * 256, ff % 256), ff % 256)

        @pl.loop(0, hidden // 512)
        def _(n):
            at = pl.ds(pl.multiple_of(n * 512, 512), 512)
            rows_in[:, at] = jnp.dot(act[...], wd[:, at], preferred_element_type=jnp.float32).astype(jnp.bfloat16)

    ret = {}
    for step in range(cp):
        xs, cs = (x + nx - order[step]) % nx, (c + cp - order[step]) % cp
        for dc, dk in col_peers:
            hop[0, step, dc, dk].wait_recv()
        for dx, dk in row_peers:
            hop[1, step, dx, dk].wait_recv()
        rows_in[0:seg] = e0[xs].reshape(seg, hidden)
        rows_in[seg:2 * seg] = e1[cs].reshape(seg, hidden)
        run_expert()
        z0[step] = rows_in[0:seg].reshape(cp, 2, cap, hidden)
        z1[step] = rows_in[seg:2 * seg].reshape(nx, 2, cap, hidden)
        for dc, dk in col_peers:
            target = device(dc, 0, dk)
            ret[0, step, dc, dk] = go(z0.at[step, target[1], (k + dk) % 2], b0.at[step, c, k], ret_y, (step, dc, dk), target)
        b0[step, c, k] = z0[step, c, k]
        for dx, dk in row_peers:
            target = device(0, dx, dk)
            ret[1, step, dx, dk] = go(z1.at[step, (x + dx) % nx, (k + dk) % 2], b1.at[step, x, k], ret_x, (step, dx, dk), target)
        b1[step, x, k] = z1[step, x, k]

    fin = {}
    for step in range(cp):
        back = order[step]
        for dc, dk in col_peers:
            ret[0, step, dc, dk].wait_recv()
        if step:
            fin[0, step] = go(b0.at[step], f0.at[x], fin_x, (step,), device(0, nx - back, 0))
        for dx, dk in row_peers:
            ret[1, step, dx, dk].wait_recv()
        if step:
            fin[1, step] = go(b1.at[step], f1.at[c], fin_y, (step,), device(cp - back, 0, 0))

    slot_f = slot_row.astype(jnp.float32)
    gates = [[jnp.transpose(jnp.broadcast_to(g_ref[b, i:i + 1, :], (tokens, tokens))) for i in range(2)] for b in range(2)]
    for step in range(cp):
        srcs = [(here[b] + order[step]) % size[b] for b in range(2)]
        picks = []
        for b in range(2):
            want = slot_f + (srcs[b] * seg).astype(jnp.float32)
            picks.append(jnp.concatenate([jnp.transpose(jnp.where(pos_ref[2 * b + i:2 * b + i + 1] == want, 1.0, 0.0)) for i in range(2)], axis=0).astype(jnp.bfloat16))
        if step:
            fin[0, step].wait_recv()
            fin[1, step].wait_recv()

        @pl.loop(0, hidden // 512)
        def _(n):
            at = pl.ds(pl.multiple_of(n * 512, 512), 512)
            for b in range(2):
                rows = (f0, f1)[b][srcs[b], :, :, :, at] if step else (b0, b1)[b][0, :, :, :, at]
                got = jnp.dot(picks[b], rows.reshape(seg, 512), preferred_element_type=jnp.float32)
                if step:
                    got += mixed[b, :, at]
                if step < cp - 1:
                    mixed[b, :, at] = got
                else:
                    g0_tile, g1_tile = (jnp.concatenate([g] * (512 // tokens), axis=1) for g in gates[b])
                    both = g0_tile * got[:tokens] + g1_tile * got[tokens:]
                    y_ref[b, :, at] = (h_ref[b, :, at].astype(jnp.float32) + both).astype(jnp.bfloat16)

    for copy in started:
        copy.wait_send()


def run_experts(mid_rows, route, gates, w_gate, w_up, w_down, cp, tp, cap):
    n_micro, tokens, hidden = mid_rows.shape
    ff = w_gate.shape[1]
    bf16 = jnp.bfloat16
    nx = tp // 2
    by_x, by_y = (cp, cp, 2, cap, hidden), (cp, nx, 2, cap, hidden)
    rows = 2 * (tp * cap)
    vmem = pl.BlockSpec(memory_space=pltpu.VMEM)
    any_spec = pl.BlockSpec(memory_space=pl.ANY)
    dma = pltpu.SemaphoreType.DMA
    return pl.pallas_call(
        functools.partial(expert_body, cp, tp, cap),
        out_shape=jax.ShapeDtypeStruct(mid_rows.shape, bf16),
        in_specs=[vmem] * 3 + [any_spec] * 3,
        out_specs=vmem,
        scratch_shapes=[pltpu.VMEM(s, jnp.float32) for s in ((8, tokens), (8, tokens), (nx, 8, tokens), (cp, 8, tokens))]
        + [pltpu.VMEM((nx, tokens, hidden), bf16), pltpu.VMEM((cp, tokens, hidden), bf16)]
        + [pltpu.VMEM(s, bf16) for s in (by_x, by_y) * 5]
        + [pltpu.VMEM((hidden, ff), bf16), pltpu.VMEM((hidden, ff), bf16), pltpu.VMEM((ff, hidden), bf16)]
        + [pltpu.VMEM((rows, hidden), bf16), pltpu.VMEM((rows, ff), bf16), pltpu.VMEM((n_micro, 2 * tokens, hidden), jnp.float32)]
        + [dma((3,)), dma((2, nx)), dma((2, cp)), dma((2, 6)), dma((2, 6)), dma((2, cp, cp, 2)), dma((2, cp, nx, 2)), dma((2, cp, cp, 2)), dma((2, cp, nx, 2)), dma((2, cp)), dma((2, cp))],
        compiler_params=pltpu.CompilerParams(collective_id=1, has_side_effects=True, vmem_limit_bytes=60 << 20),
        cost_estimate=pl.CostEstimate(flops=6 * 4 * rows * hidden * ff, bytes_accessed=6 * hidden * ff, transcendentals=0),
    )(mid_rows, route, gates, w_gate, w_up, w_down)


def hand_out_body(src, dst):
    dst[...] = src[...]


def hand_out(rows):
    vmem = pl.BlockSpec((1,) + rows.shape[1:], lambda i: (i, 0, 0))
    return pl.pallas_call(hand_out_body, grid=rows.shape[:1], out_shape=jax.ShapeDtypeStruct(rows.shape, rows.dtype), in_specs=[vmem], out_specs=vmem)(rows)


def solution(mesh):
    cp_size = mesh.shape['cp']
    tp_size = mesh.shape['tp']
    experts = cp_size * tp_size
    row_spec = P(None, ('data', 'cp', 'tp'), None)
    head_spec = P(None, 'tp', None)
    out_spec = P('tp', None, None)
    expert_spec = P(('cp', 'tp'), None, None)

    def device_step(act_in, route_ids, route_gates, w_query, w_key, w_value, w_out, w_gate, w_up, w_down):
        n_micro, tokens, hidden = act_in.shape
        heads, head_dim = w_query.shape[1], w_query.shape[2]
        mid_rows = run_front(act_in, w_query, w_key, w_value, w_out, cp_size, tp_size, heads)

        capacity = (4 * tokens) // experts
        route = jnp.transpose(route_ids, (0, 2, 1))
        gates = jnp.transpose(route_gates, (0, 2, 1))
        rows_out = run_experts(mid_rows, route, gates, w_gate[0], w_up[0], w_down[0], cp_size, tp_size, capacity)
        return hand_out(rows_out)

    return jax.shard_map(device_step, mesh=mesh, in_specs=(row_spec, row_spec, row_spec, head_spec, head_spec, head_spec, out_spec, expert_spec, expert_spec, expert_spec), out_specs=row_spec, check_vma=False)
```
